32 devices in a mesh: rep: 2 (over x), slab: 8 (over z, y), pix: 2 (over core).
Axes of the slice: x: 2, y: 2, z: 4, core: 2. Of those that a mesh axis runs over, the one named last changes fastest.
Arguments:
- projections: bfloat16 [16, 256, 512], P(('rep', 'pix'), 'slab'), may hold values from -6 to 6
- ctf_weight: bfloat16 [16, 256, 256], P(('rep', 'pix'), 'slab'), may hold values from 0.099609375 to 4
- orient: int32 [16], P(('rep', 'pix')), may hold values from 0 to 63
- angle_table: int32 [64, 4, 256], replicated, may hold values from 0 to 255, as said below
Outputs:
- density: float32 [256, 256, 512], P(('rep', 'pix'), 'slab')
The draws below stay inside these ranges and needn't reach their ends.
Inputs may be any that keep to these rules, and one draw needn't show every extreme that they name: `angle_table`: for every entry and column, the lower indices lie between 3 and 253, and the fractions between 0 and 255.
All inputs are finite; a program needn't handle non-finite values.
Results may differ from the reference program's by a relative error of at most 0.0022.
Values may be sent and summed in bfloat16 or wider, within the bound.
No kernel may reach another device: no remote copies, remote signals or barrier semaphores. Data moves between devices by JAX's collectives and lax.ppermute only.
A program may use at most 128 MiB of HBM per device.

```python
import math
import jax
import jax.numpy as jnp
from jax import lax

GRID = 256
ANGLES = 64
NPROJ = 16


def draw_angle_table(key, part):
    center = GRID // 2
    reach = 256 * (center - 3) // center
    sines = jax.random.randint(key, (ANGLES,), -reach, reach + 1)
    remain = reach * reach - sines * sines
    counter = jnp.arange(1, reach + 1, dtype=jnp.int32)
    cosines = jnp.sum((counter[None, :] * counter[None, :] <= remain[:, None]).astype(jnp.int32), axis=1)
    offsets = jnp.arange(GRID, dtype=jnp.int32) - center
    position_x = center * 256 + offsets[None, :] * cosines[:, None]
    position_z = center * 256 + offsets[None, :] * sines[:, None]
    return jnp.stack([position_x // 256, position_x % 256, position_z // 256, position_z % 256], axis=1).astype(jnp.int32)


def plant(array, stream_key, least, top_value):
    place = [jax.random.randint(jax.random.fold_in(stream_key, axis), (), 0, length) for axis, length in enumerate(array.shape)]
    widest = array.shape.index(max(array.shape))
    neighbour = place[:widest] + [(place[widest] + 1) % array.shape[widest]] + place[widest + 1:]
    return array.at[tuple(place)].set(least).at[tuple(neighbour)].set(top_value)


def level_of(rng, shape, cuts, smallest, largest):
    factor_of, own = 1.0, jax.random.fold_in(rng, 6)
    for dim, parts in cuts:
        steps = jnp.exp(jax.random.uniform(jax.random.fold_in(own, dim), (parts,), jnp.float32, smallest / len(cuts), largest / len(cuts)))
        factor_of = factor_of * jnp.repeat(steps, shape[dim] // parts).reshape([-1 if axis == dim else 1 for axis in range(len(shape))])
    return factor_of


def gaussian(stream_key, shape, spread, most, cuts=(), kind=jnp.bfloat16):
    result = jax.random.normal(stream_key, shape, jnp.float32) * spread
    if len(cuts) > 0:
        result = level_of(stream_key, shape, cuts, -0.22, 0.18) * result
    return jnp.clip(result, min=-most, max=most).astype(kind)


def setup_inputs(seed: int = 0) -> dict:
    streams_of = jax.random.split(jax.random.key(seed), 5)
    projections = gaussian(streams_of[0], (NPROJ, GRID, 2 * GRID), 1.0, 6.0, ((0, 4), (1, 8)))
    ctf_weight = jnp.clip(jnp.exp(math.log(4.0) - 3.6927934 * jax.random.uniform(streams_of[1], (NPROJ, GRID, GRID), jnp.float32) ** level_of(streams_of[1], (NPROJ, GRID, GRID), ((0, 4), (1, 8)), -0.2, 0.2)), 0.099609375, 4.0).astype(jnp.bfloat16)
    orient = plant(jax.random.randint(streams_of[2], (NPROJ,), 0, ANGLES), jax.random.fold_in(streams_of[2], 1), 0, ANGLES - 1).astype(jnp.int32)
    angle_table = draw_angle_table(jax.random.fold_in(streams_of[4], 71), 0)
    return {"projections": projections, "ctf_weight": ctf_weight, "orient": orient, "angle_table": angle_table}


def reference(projections, ctf_weight, orient, angle_table):
    samples = jnp.concatenate([projections, ctf_weight], axis=2).astype(jnp.float32)
    geometry = angle_table[orient]
    volume = jnp.zeros((GRID, GRID, 3 * GRID), jnp.float32)

    def add_one(running, item):
        rows_in, where = item
        lower_x = where[0].astype(jnp.int32)
        lower_z = where[2].astype(jnp.int32)
        share_x = where[1].astype(jnp.float32) / 256.0
        share_z = where[3].astype(jnp.float32) / 256.0
        for step_x, weight_x in ((0, 1.0 - share_x), (1, share_x)):
            for step_z, weight_z in ((0, 1.0 - share_z), (1, share_z)):
                coeff = (weight_x * weight_z).astype(jnp.bfloat16).astype(jnp.float32)
                running = running.at[lower_x + step_x, lower_z + step_z].add(coeff[:, None] * rows_in)
        return running, None

    volume, _ = lax.scan(add_one, volume, (samples, geometry))
    values = volume[:, :, :2 * GRID].reshape(GRID, GRID, 2, GRID)
    weights = volume[:, :, None, 2 * GRID:] + 1.0
    return (values / weights).reshape(GRID, GRID, 2 * GRID)
```

```python
import jax
import jax.numpy as jnp
import numpy as np
from jax import lax
from jax.experimental import pallas as pl
from jax.experimental.pallas import tpu as pltpu
from jax.sharding import PartitionSpec as P

BATCH_AXES = ("rep", "pix")
GROUP = 16
TILE = 256
LANES = 128

SCHEDULE = (
    ("x", "100", "000"), ("y", "010", "000"), ("z", "001", "000"),
    ("x", "101", "001"), ("y", "110", "100"), ("z", "002", "001"),
    ("x", "102", "002"), ("y", "012", "002"), ("z", "003", "002"),
    ("x", "103", "003"), ("y", "013", "003"), ("z", "111", "110"),
    ("x", "113", "013"), ("y", "011", "001"), ("z", "112", "111"),
)


class Ports:
    def __init__(self, mesh):
        self.rep, self.slab, self.pix = (mesh.shape[a] for a in ("rep", "slab", "pix"))

    def fits(self):
        return (self.rep, self.slab, self.pix) == (2, 8, 2)

    def pairs(self, port):
        if port == "x":
            return "rep", [(i, 1 - i) for i in range(self.rep)]
        if port == "y":
            return "slab", [(i, i ^ 1) for i in range(self.slab)]
        if port == "z":
            return "slab", [(i, (i + 2) % self.slab) for i in range(self.slab)]
        return "pix", [(i, 1 - i) for i in range(self.pix)]

    def send(self, value, port):
        axis, pairs = self.pairs(port)
        return lax.ppermute(value, axis, pairs)

    def move(self, owner, port):
        axis, pairs = self.pairs(port)
        dim = ("rep", "slab", "pix").index(axis)
        moved = np.empty_like(owner)
        for source, target in pairs:
            to, frm = [slice(None)] * 3, [slice(None)] * 3
            to[dim], frm[dim] = target, source
            moved[tuple(to)] = owner[tuple(frm)]
        return moved


def gather_pieces(samples, ports):
    first = np.arange(ports.rep * ports.slab * ports.pix).reshape(ports.rep, ports.slab, ports.pix)
    held = {"000": (samples, first)}
    for port, name, source in SCHEDULE:
        value, owner = held[source]
        held[name] = (ports.send(value, port), ports.move(owner, port))
    pieces = list(held.values())
    pieces += [(ports.send(v, "core"), ports.move(o, "core")) for v, o in pieces]
    owners = np.stack([o for _, o in pieces], axis=-1)
    assert (np.sort(owners, -1) == np.arange(first.size)).all()
    return [v for v, _ in pieces], owners


def lookup(orient, angle_table):
    choose = (orient[:, None] == lax.iota(jnp.int32, angle_table.shape[0])[None, :]).astype(jnp.int32)
    return jnp.sum(choose[:, :, None, None] * angle_table[None], axis=1)


def corner(indices, lower, fraction):
    return jnp.where(indices == lower, 1.0 - fraction, 0.0) + jnp.where(indices == lower + 1, fraction, 0.0)


def spread(pieces, place, active, geometry, box, count_x, count_z, columns, per_piece):
    batch, width = per_piece
    pieces_n = len(pieces)
    groups = width // GROUP
    segments = pieces_n * batch * groups
    rows_max = segments * GROUP
    row_block = TILE // count_z
    steps = count_x // row_block
    channels = 3 * columns
    lane_groups = LANES // GROUP

    def kernel(*refs):
        box_ref, place_ref, active_ref, geometry_ref = refs[:4]
        piece_refs = refs[4 : 4 + pieces_n]
        out_ref = refs[4 + pieces_n]
        compact, listed, where, total, staged, sems = refs[5 + pieces_n :]
        first_x, first_z = box_ref[0], box_ref[1]

        count = jnp.int32(0)
        for index, piece in enumerate(piece_refs):
            first_n, first_group = place_ref[2 * index], place_ref[2 * index + 1]

            def take(item, count, piece=piece, first_n=first_n, first_group=first_group):
                name = (first_n + item // groups) * (columns // GROUP) + first_group + item % groups
                hit = active_ref[name]

                @pl.when(hit > 0)
                def _():
                    source = pl.ds(pl.multiple_of(item * GROUP, GROUP), GROUP)
                    target = pl.ds(pl.multiple_of(count * GROUP, GROUP), GROUP)
                    compact[target, :] = piece[source, :]
                    listed[count] = name

                return count + hit

            count = lax.fori_loop(0, batch * groups, take, count)

        tiles = (count * GROUP + TILE - 1) // TILE

        def clear(item, carry):
            target = pl.ds(pl.multiple_of(item * GROUP, GROUP), GROUP)
            compact[target, :] = jnp.zeros((GROUP, channels), jnp.bfloat16)
            return carry

        lax.fori_loop(count, tiles * (TILE // GROUP), clear, 0)

        lane_group = lax.broadcasted_iota(jnp.int32, (8, LANES), 1) // GROUP

        def order(block, carry):
            gathered = jnp.full((8, LANES), -4.0, jnp.float32)
            for slot in range(lane_groups):
                item = block * lane_groups + slot
                valid = item < count
                name = listed[jnp.minimum(item, count - 1)]
                n, group = name // (columns // GROUP), name % (columns // GROUP)
                lanes = pl.ds(pl.multiple_of(group // lane_groups * LANES, LANES), LANES)
                source = geometry_ref[n, :, lanes]
                shift = lax.rem(slot - lax.rem(group, lane_groups) + lane_groups, lane_groups) * GROUP
                rolled = pltpu.roll(source, shift, 1)
                gathered = jnp.where((lane_group == slot) & valid, rolled, gathered)
            where[:, pl.ds(pl.multiple_of(block * LANES, LANES), LANES)] = gathered
            return carry

        lax.fori_loop(0, tiles * (TILE // LANES), order, 0)

        def out_copy(step, slot):
            rows = pl.ds(step * row_block, row_block)
            return pltpu.make_async_copy(staged.at[slot], out_ref.at[rows], sems.at[slot])

        for step in range(steps):
            slot = step % 2
            total[...] = jnp.zeros_like(total)

            def add(tile, carry, step=step):
                lanes = pl.ds(pl.multiple_of(tile * TILE, TILE), TILE)
                lower_x, part_x = where[0:1, lanes], where[1:2, lanes]
                lower_z, part_z = where[2:3, lanes], where[3:4, lanes]
                at_x = (first_x + step * row_block + lax.broadcasted_iota(jnp.int32, (row_block, TILE), 0)).astype(jnp.float32)
                at_z = (first_z + lax.broadcasted_iota(jnp.int32, (count_z, TILE), 0)).astype(jnp.float32)
                weight_x = corner(at_x, lower_x, part_x)
                weight_z = corner(at_z, lower_z, part_z)
                matrix = (weight_x[:, None, :] * weight_z[None, :, :]).astype(jnp.bfloat16)
                matrix = matrix.reshape(row_block * count_z, TILE)
                total[...] += jnp.dot(matrix, compact[lanes, :], preferred_element_type=jnp.float32)
                return carry

            lax.fori_loop(0, tiles, add, 0)
            if step >= 2:
                out_copy(step - 2, slot).wait()
            scale = 1.0 / (total[:, 2 * columns :] + 1.0)
            shape = (row_block, count_z, columns)
            staged[slot, :, :, :columns] = (total[:, :columns] * scale).reshape(shape)
            staged[slot, :, :, columns:] = (total[:, columns : 2 * columns] * scale).reshape(shape)
            out_copy(step, slot).start()
        for step in range(max(steps - 2, 0), steps):
            out_copy(step, step % 2).wait()

    smem, vmem = pl.BlockSpec(memory_space=pltpu.SMEM), pl.BlockSpec(memory_space=pltpu.VMEM)
    return pl.pallas_call(
        kernel,
        out_shape=jax.ShapeDtypeStruct((count_x, count_z, 2 * columns), jnp.float32),
        in_specs=[smem, smem, smem, vmem] + [vmem] * pieces_n,
        out_specs=pl.BlockSpec(memory_space=pl.ANY),
        scratch_shapes=[
            pltpu.VMEM((rows_max, channels), jnp.bfloat16),
            pltpu.SMEM((segments,), jnp.int32),
            pltpu.VMEM((8, rows_max), jnp.float32),
            pltpu.VMEM((row_block * count_z, channels), jnp.float32),
            pltpu.VMEM((2, row_block, count_z, 2 * columns), jnp.float32),
            pltpu.SemaphoreType.DMA((2,)),
        ],
        compiler_params=pltpu.CompilerParams(vmem_limit_bytes=20 << 20),
        name="spread",
    )(box, place, active, geometry, *pieces)


def make_body(ports):
    def body(projections, ctf_weight, orient, angle_table):
        batch, planes = projections.shape[:2]
        columns = projections.shape[2] // 2
        owned_rows = columns // (ports.rep * ports.pix)
        first_z = lax.axis_index("slab") * planes
        first_x = (lax.axis_index("rep") * ports.pix + lax.axis_index("pix")) * owned_rows
        samples = jnp.concatenate([projections, ctf_weight], axis=2).reshape(batch * planes, 3 * columns)
        pieces, owners = gather_pieces(samples, ports)

        geometry = lookup(lax.all_gather(orient, BATCH_AXES, axis=0, tiled=True), angle_table)
        lower_x, lower_z = geometry[:, 0], geometry[:, 2]
        hit = (lower_x >= first_x - 1) & (lower_x < first_x + owned_rows)
        hit &= (lower_z >= first_z - 1) & (lower_z < first_z + planes)
        active = jnp.any(hit.reshape(-1, GROUP), axis=1).astype(jnp.int32)
        unit = jnp.array([1.0, 1.0 / 256.0, 1.0, 1.0 / 256.0], jnp.float32)
        table = jnp.pad(geometry.astype(jnp.float32) * unit[None, :, None], ((0, 0), (0, 4), (0, 0)))

        owner_rep, owner_slab, owner_pix = np.unravel_index(owners, owners.shape[:3])
        place = np.stack([(owner_rep * ports.pix + owner_pix) * batch, owner_slab * (planes // GROUP)], -1)
        place = jnp.asarray(place.reshape(-1, place.shape[-2] * 2), jnp.int32)
        me = (lax.axis_index("rep") * ports.slab + lax.axis_index("slab")) * ports.pix + lax.axis_index("pix")
        place = lax.dynamic_index_in_dim(place, me, 0, keepdims=False)
        box = jnp.stack([first_x, first_z]).astype(jnp.int32)
        return spread(pieces, place, active, table, box, owned_rows, planes, columns, (batch, planes))

    return body


def plain_body(projections, ctf_weight, orient, angle_table):
    planes = projections.shape[1]
    columns = projections.shape[2] // 2
    owned_rows = columns // (lax.axis_size("rep") * lax.axis_size("pix"))
    first_z = lax.axis_index("slab") * planes
    first_x = (lax.axis_index("rep") * lax.axis_size("pix") + lax.axis_index("pix")) * owned_rows
    samples = jnp.concatenate([projections, ctf_weight], axis=2)
    samples = lax.all_gather(samples, "slab", axis=1, tiled=True)
    samples = lax.all_gather(samples, BATCH_AXES, axis=0, tiled=True)
    geometry = lookup(lax.all_gather(orient, BATCH_AXES, axis=0, tiled=True), angle_table)
    geometry = geometry.astype(jnp.float32)
    at_x = (first_x + lax.iota(jnp.int32, owned_rows)).astype(jnp.float32)[:, None, None]
    at_z = (first_z + lax.iota(jnp.int32, planes)).astype(jnp.float32)[:, None, None]
    weight_x = corner(at_x, geometry[None, :, 0], geometry[None, :, 1] / 256.0)
    weight_z = corner(at_z, geometry[None, :, 2], geometry[None, :, 3] / 256.0)
    matrix = (weight_x[:, None] * weight_z[None]).astype(jnp.bfloat16).reshape(owned_rows * planes, -1)
    volume = jnp.dot(matrix, samples.reshape(-1, 3 * columns), preferred_element_type=jnp.float32)
    values = volume[:, : 2 * columns].reshape(-1, 2, columns) / (volume[:, None, 2 * columns :] + 1.0)
    return values.reshape(owned_rows, planes, 2 * columns)


def solution(mesh):
    placed = (
        P(BATCH_AXES, "slab", None),
        P(BATCH_AXES, "slab", None),
        P(BATCH_AXES),
        P(),
    )
    ports = Ports(mesh)
    body = make_body(ports) if ports.fits() else plain_body
    return jax.shard_map(
        body, mesh=mesh, in_specs=placed, out_specs=P(BATCH_AXES, "slab", None), check_vma=False
    )
```

```python
import jax
import jax.numpy as jnp
import numpy as np
from jax import lax
from jax.experimental import pallas as pl
from jax.experimental.pallas import tpu as pltpu
from jax.sharding import PartitionSpec as P

BATCH_AXES = ("rep", "pix")
GROUP = 16
TILE = 256
LANES = 128

SCHEDULE = (
    ("z", "001", "000"), ("x", "100", "000"), ("y", "010", "000"),
    ("back", "003", "000"), ("xy", "110", "000"),
    ("z", "002", "001"), ("x", "101", "001"), ("y", "011", "001"),
    ("z", "111", "110"), ("x", "103", "003"), ("y", "013", "003"),
    ("back", "113", "110"), ("x", "102", "002"), ("y", "012", "002"),
    ("z", "112", "111"),
)


class Ports:
    def __init__(self, mesh):
        self.rep, self.slab, self.pix = (mesh.shape[a] for a in ("rep", "slab", "pix"))
        self.ids = np.arange(self.rep * self.slab * self.pix).reshape(self.rep, self.slab, self.pix)

    def fits(self):
        return (self.rep, self.slab, self.pix) == (2, 8, 2)

    def target(self, port, rep, slab, pix):
        if port in ("x", "xy"):
            rep = 1 - rep
        if port in ("y", "xy"):
            slab = slab ^ 1
        if port == "z":
            slab = (slab + 2) % self.slab
        if port == "back":
            slab = (slab - 2) % self.slab
        if port == "core":
            pix = 1 - pix
        return self.ids[rep, slab, pix]

    def pairs(self, port):
        return [(int(self.ids[at]), int(self.target(port, *at))) for at in np.ndindex(self.ids.shape)]

    def send(self, value, port):
        return lax.ppermute(value, ("rep", "slab", "pix"), self.pairs(port))

    def move(self, owner, port):
        moved = np.empty_like(owner)
        for source, target in self.pairs(port):
            moved.flat[target] = owner.flat[source]
        return moved


def gather_pieces(samples, ports):
    held = {"000": (samples, ports.ids)}
    for port, name, source in SCHEDULE:
        value, owner = held[source]
        held[name] = (ports.send(value, port), ports.move(owner, port))
    pieces = list(held.values())
    pieces += [(ports.send(v, "core"), ports.move(o, "core")) for v, o in pieces]
    owners = np.stack([o for _, o in pieces], axis=-1)
    assert (np.sort(owners, -1) == np.arange(ports.ids.size)).all()
    return [v for v, _ in pieces], owners


def lookup(orient, angle_table):
    choose = (orient[:, None] == lax.iota(jnp.int32, angle_table.shape[0])[None, :]).astype(jnp.int32)
    return jnp.sum(choose[:, :, None, None] * angle_table[None], axis=1)


def corner(indices, lower, fraction):
    return jnp.where(indices == lower, 1.0 - fraction, 0.0) + jnp.where(indices == lower + 1, fraction, 0.0)


def make_plan(orient, place, table, pieces_n, sizes):
    batch, planes, columns, count_x, row_block, batches = sizes
    groups, items = columns // GROUP, batch * planes // GROUP
    segments = pieces_n * items
    steps, lane_groups = count_x // row_block, LANES // GROUP
    bits_at = 2 * segments
    info_size = segments + segments * GROUP // TILE + 1
    total_n = batch * batches

    def kernel(orient_ref, place_ref, table_ref, info_ref, where_ref, geometry, found, found_s, listed, sems):
        rep, pix = lax.axis_index("rep"), lax.axis_index("pix")
        first_x = (rep * lax.axis_size("pix") + pix) * count_x
        first_z = lax.axis_index("slab") * planes
        copies = [
            pltpu.make_async_copy(table_ref.at[orient_ref[n]], geometry.at[place_ref[n]], sems.at[n])
            for n in range(total_n)
        ]
        for copy in copies:
            copy.start()
        for copy in copies:
            copy.wait()
        near_x = geometry[:, 0, :] - first_x.astype(jnp.float32)
        near_z = geometry[:, 2, :] - first_z.astype(jnp.float32)
        hit_z = (near_z >= -1.0) & (near_z < planes)
        hits = [
            jnp.where(hit_z & (near_x >= s * row_block - 1.0) & (near_x < (s + 1) * row_block), 1.0, 0.0)
            for s in range(steps)
        ]
        hits = jnp.concatenate(hits, axis=0).astype(jnp.bfloat16)
        lane = lax.broadcasted_iota(jnp.int32, (columns, LANES), 0)
        group = lax.broadcasted_iota(jnp.int32, (columns, LANES), 1)
        member = (lane // GROUP == group).astype(jnp.bfloat16)
        counted = jnp.dot(hits, member, preferred_element_type=jnp.float32)
        bits = jnp.zeros((total_n, LANES), jnp.float32)
        for s in range(steps):
            bits += jnp.where(counted[s * total_n : (s + 1) * total_n] > 0.0, float(2**s), 0.0)
        any_hit = jnp.where(bits > 0.0, 1.0, 0.0).astype(jnp.bfloat16)
        row = lax.broadcasted_iota(jnp.int32, (total_n, total_n), 0)
        col = lax.broadcasted_iota(jnp.int32, (total_n, total_n), 1)
        above = jnp.dot((col < row).astype(jnp.bfloat16), any_hit, preferred_element_type=jnp.float32)
        whole = jnp.dot(jnp.ones((total_n, total_n), jnp.bfloat16), any_hit, preferred_element_type=jnp.float32)
        row = lax.broadcasted_iota(jnp.int32, (LANES, LANES), 0)
        col = lax.broadcasted_iota(jnp.int32, (LANES, LANES), 1)
        before = jnp.dot(
            whole.astype(jnp.bfloat16), (row < col).astype(jnp.bfloat16), preferred_element_type=jnp.float32
        )
        code = jnp.where(bits > 0.0, bits * bits_at + above + before, 0.0)
        found[...] = code.astype(jnp.int32)
        to_scalar = pltpu.make_async_copy(found, found_s, sems.at[0])
        to_scalar.start()
        to_scalar.wait()

        for tile in range(segments, info_size):
            info_ref[tile] = 0

        def note(index, count):
            piece, item = index // items, index % items
            n = place_ref[total_n + 2 * piece] + item // (items // batch)
            g = place_ref[total_n + 2 * piece + 1] + item % (items // batch)
            code = found_s[n, g]
            hit = code > 0
            slot = jnp.where(hit, lax.rem(code, bits_at), segments)
            info_ref[index] = jnp.where(hit, code, segments)
            listed[slot] = n * groups + g
            tile = segments + jnp.where(hit, slot * GROUP // TILE, 0)
            info_ref[tile] = info_ref[tile] | (code // bits_at)
            return count + hit.astype(jnp.int32)

        count = lax.fori_loop(0, segments, note, jnp.int32(0))
        info_ref[info_size - 1] = count
        tiles = (count * GROUP + TILE - 1) // TILE
        lane_group = lax.broadcasted_iota(jnp.int32, (8, LANES), 1) // GROUP

        def order(block, carry):
            gathered = jnp.full((8, LANES), -4.0, jnp.float32)
            for slot in range(lane_groups):
                index = block * lane_groups + slot
                valid = index < count
                name = listed[jnp.minimum(index, count - 1)]
                n, g = name // groups, name % groups
                lanes = pl.ds(pl.multiple_of(g // lane_groups * LANES, LANES), LANES)
                shift = lax.rem(slot - lax.rem(g, lane_groups) + lane_groups, lane_groups) * GROUP
                rolled = pltpu.roll(geometry[n, :, lanes], shift, 1)
                gathered = jnp.where((lane_group == slot) & valid, rolled, gathered)
            where_ref[:, pl.ds(pl.multiple_of(block * LANES, LANES), LANES)] = gathered
            return carry

        lax.fori_loop(0, tiles * (TILE // LANES), order, 0)

    smem, vmem = pl.BlockSpec(memory_space=pltpu.SMEM), pl.BlockSpec(memory_space=pltpu.VMEM)
    return pl.pallas_call(
        kernel,
        out_shape=[
            jax.ShapeDtypeStruct((info_size,), jnp.int32),
            jax.ShapeDtypeStruct((8, segments * GROUP), jnp.float32),
        ],
        in_specs=[smem, smem, pl.BlockSpec(memory_space=pl.ANY)],
        out_specs=[smem, vmem],
        scratch_shapes=[
            pltpu.VMEM((total_n, 8, columns), jnp.float32),
            pltpu.VMEM((total_n, LANES), jnp.int32),
            pltpu.SMEM((total_n, LANES), jnp.int32),
            pltpu.SMEM((segments + 1,), jnp.int32),
            pltpu.SemaphoreType.DMA((total_n,)),
        ],
        compiler_params=pltpu.CompilerParams(vmem_limit_bytes=4 << 20),
        name="plan",
    )(orient, place, table)


def spread(pieces, info, where, sizes):
    batch, planes, columns, count_x, row_block, batches = sizes
    pieces_n = len(pieces)
    items = batch * planes // GROUP
    segments = pieces_n * items
    bits_at = 2 * segments
    steps = count_x // row_block
    channels = 3 * columns

    def kernel(*refs):
        info_ref, where_ref = refs[:2]
        piece_refs = refs[2 : 2 + pieces_n]
        out_ref = refs[2 + pieces_n]
        compact, total, staged, sems = refs[3 + pieces_n :]
        first_x = (lax.axis_index("rep") * lax.axis_size("pix") + lax.axis_index("pix")) * count_x
        first_z = lax.axis_index("slab") * planes
        count = info_ref[segments + segments * GROUP // TILE]
        tiles = (count * GROUP + TILE - 1) // TILE

        for index, piece in enumerate(piece_refs):
            codes = [info_ref[index * items + item] for item in range(items)]
            most = codes[0]
            for code in codes[1:]:
                most = jnp.maximum(most, code)

            @pl.when(most > segments)
            def _(codes=codes, piece=piece):
                for item, code in enumerate(codes):
                    target = pl.ds(pl.multiple_of(lax.rem(code, bits_at) * GROUP, GROUP), GROUP)
                    compact[target, :] = piece[item * GROUP : (item + 1) * GROUP, :]

        def clear(item, carry):
            target = pl.ds(pl.multiple_of(item * GROUP, GROUP), GROUP)
            compact[target, :] = jnp.zeros((GROUP, channels), jnp.bfloat16)
            return carry

        lax.fori_loop(count, tiles * (TILE // GROUP), clear, 0)

        def out_copy(step, slot):
            rows = pl.ds(step * row_block, row_block)
            return pltpu.make_async_copy(staged.at[slot], out_ref.at[rows], sems.at[slot])

        for step in range(steps):
            slot = step % 2

            def product(tile, step=step):
                lanes = pl.ds(pl.multiple_of(tile * TILE, TILE), TILE)
                lower_x, part_x = where_ref[0:1, lanes], where_ref[1:2, lanes]
                lower_z, part_z = where_ref[2:3, lanes], where_ref[3:4, lanes]
                at_x = first_x + step * row_block + lax.broadcasted_iota(jnp.int32, (row_block, TILE), 0)
                at_z = first_z + lax.broadcasted_iota(jnp.int32, (planes, TILE), 0)
                weight_x = corner(at_x.astype(jnp.float32), lower_x, part_x)
                weight_z = corner(at_z.astype(jnp.float32), lower_z, part_z)
                matrix = (weight_x[:, None, :] * weight_z[None, :, :]).astype(jnp.bfloat16)
                matrix = matrix.reshape(row_block * planes, TILE)
                return jnp.dot(matrix, compact[lanes, :], preferred_element_type=jnp.float32)

            def add(tile, seen, step=step, product=product):
                hit = lax.rem(info_ref[segments + tile] // 2**step, 2)

                @pl.when((hit > 0) & (seen == 0))
                def _():
                    total[...] = product(tile)

                @pl.when((hit > 0) & (seen > 0))
                def _():
                    total[...] += product(tile)

                return seen + hit

            seen = lax.fori_loop(0, tiles, add, jnp.int32(0))
            if step >= 2:
                out_copy(step - 2, slot).wait()
            shape = (row_block, planes, columns)

            @pl.when(seen > 0)
            def _(slot=slot):
                scale = 1.0 / (total[:, 2 * columns :] + 1.0)
                staged[slot, :, :, :columns] = (total[:, :columns] * scale).reshape(shape)
                staged[slot, :, :, columns:] = (total[:, columns : 2 * columns] * scale).reshape(shape)

            @pl.when(seen == 0)
            def _(slot=slot):
                staged[slot] = jnp.zeros((row_block, planes, 2 * columns), jnp.float32)

            out_copy(step, slot).start()
        for step in range(max(steps - 2, 0), steps):
            out_copy(step, step % 2).wait()

    smem, vmem = pl.BlockSpec(memory_space=pltpu.SMEM), pl.BlockSpec(memory_space=pltpu.VMEM)
    return pl.pallas_call(
        kernel,
        out_shape=jax.ShapeDtypeStruct((count_x, planes, 2 * columns), jnp.float32),
        in_specs=[smem, vmem] + [vmem] * pieces_n,
        out_specs=pl.BlockSpec(memory_space=pl.ANY),
        scratch_shapes=[
            pltpu.VMEM((segments * GROUP + GROUP, channels), jnp.bfloat16),
            pltpu.VMEM((row_block * planes, channels), jnp.float32),
            pltpu.VMEM((2, row_block, planes, 2 * columns), jnp.float32),
            pltpu.SemaphoreType.DMA((2,)),
        ],
        compiler_params=pltpu.CompilerParams(vmem_limit_bytes=14 << 20),
        name="spread",
    )(info, where, *pieces)


def make_body(ports):
    def body(projections, ctf_weight, orient, angle_table):
        batch, planes = projections.shape[:2]
        columns = projections.shape[2] // 2
        count_x = columns // (ports.rep * ports.pix)
        row_block = TILE // planes
        sizes = (batch, planes, columns, count_x, row_block, ports.rep * ports.pix)
        samples = jnp.concatenate([projections, ctf_weight], axis=2).reshape(batch * planes, 3 * columns)
        pieces, owners = gather_pieces(samples, ports)

        across = ports.send(orient, "x")
        orients = [orient, across, ports.send(orient, "core"), ports.send(across, "core")]
        relative = [ports.ids, ports.move(ports.ids, "x")]
        relative += [ports.move(o, "core") for o in relative]
        order = np.stack([np.stack(np.unravel_index(o, o.shape)) for o in relative], axis=-1)
        order = (order[0] * ports.pix + order[2])[..., None] * batch + np.arange(batch)

        owner_rep, owner_slab, owner_pix = np.unravel_index(owners, ports.ids.shape)
        place = np.stack([(owner_rep * ports.pix + owner_pix) * batch, owner_slab * (planes // GROUP)], -1)
        place = np.concatenate([order.reshape(ports.ids.size, -1), place.reshape(ports.ids.size, -1)], axis=1)
        me = (lax.axis_index("rep") * ports.slab + lax.axis_index("slab")) * ports.pix + lax.axis_index("pix")
        place = lax.dynamic_index_in_dim(jnp.asarray(place, jnp.int32), me, 0, keepdims=False)
        unit = jnp.array([1.0, 1.0 / 256.0, 1.0, 1.0 / 256.0], jnp.float32)
        table = jnp.pad(angle_table.astype(jnp.float32) * unit[None, :, None], ((0, 0), (0, 4), (0, 0)))
        info, where = make_plan(jnp.concatenate(orients), place, table, len(pieces), sizes)
        return spread(pieces, info, where, sizes)

    return body


def plain_body(projections, ctf_weight, orient, angle_table):
    planes = projections.shape[1]
    columns = projections.shape[2] // 2
    owned_rows = columns // (lax.axis_size("rep") * lax.axis_size("pix"))
    first_z = lax.axis_index("slab") * planes
    first_x = (lax.axis_index("rep") * lax.axis_size("pix") + lax.axis_index("pix")) * owned_rows
    samples = jnp.concatenate([projections, ctf_weight], axis=2)
    samples = lax.all_gather(samples, "slab", axis=1, tiled=True)
    samples = lax.all_gather(samples, BATCH_AXES, axis=0, tiled=True)
    geometry = lookup(lax.all_gather(orient, BATCH_AXES, axis=0, tiled=True), angle_table)
    geometry = geometry.astype(jnp.float32)
    at_x = (first_x + lax.iota(jnp.int32, owned_rows)).astype(jnp.float32)[:, None, None]
    at_z = (first_z + lax.iota(jnp.int32, planes)).astype(jnp.float32)[:, None, None]
    weight_x = corner(at_x, geometry[None, :, 0], geometry[None, :, 1] / 256.0)
    weight_z = corner(at_z, geometry[None, :, 2], geometry[None, :, 3] / 256.0)
    matrix = (weight_x[:, None] * weight_z[None]).astype(jnp.bfloat16).reshape(owned_rows * planes, -1)
    volume = jnp.dot(matrix, samples.reshape(-1, 3 * columns), preferred_element_type=jnp.float32)
    values = volume[:, : 2 * columns].reshape(-1, 2, columns) / (volume[:, None, 2 * columns :] + 1.0)
    return values.reshape(owned_rows, planes, 2 * columns)


def solution(mesh):
    placed = (
        P(BATCH_AXES, "slab", None),
        P(BATCH_AXES, "slab", None),
        P(BATCH_AXES),
        P(),
    )
    ports = Ports(mesh)
    body = make_body(ports) if ports.fits() else plain_body
    return jax.shard_map(
        body, mesh=mesh, in_specs=placed, out_specs=P(BATCH_AXES, "slab", None), check_vma=False
    )
```

```python
import jax
import jax.numpy as jnp
import numpy as np
from jax import lax
from jax.experimental import pallas as pl
from jax.experimental.pallas import tpu as pltpu
from jax.sharding import PartitionSpec as P


BATCH_AXES = ("rep", "pix")
GROUP = 16
TILE = 256
LANES = 128


class Ports:
    def __init__(self, mesh):
        self.rep, self.slab, self.pix = (mesh.shape[a] for a in ("rep", "slab", "pix"))
        self.ids = np.arange(self.rep * self.slab * self.pix).reshape(self.rep, self.slab, self.pix)

    def fits(self):
        return (self.rep, self.slab, self.pix) == (2, 8, 2)

    def target(self, port, rep, slab, pix):
        if port == "x|y":
            port = "y" if pix else "x"
        if port in ("x", "xy"):
            rep = 1 - rep
        if port in ("y", "xy"):
            slab = slab ^ 1
        if port == "z":
            slab = (slab + 2) % self.slab
        if port == "back":
            slab = (slab - 2) % self.slab
        if port == "core":
            pix = 1 - pix
        return self.ids[rep, slab, pix]

    def pairs(self, port):
        return [(int(self.ids[at]), int(self.target(port, *at))) for at in np.ndindex(self.ids.shape)]

    def move(self, owner, port):
        moved = np.empty_like(owner)
        for source, target in self.pairs(port):
            moved.flat[target] = owner.flat[source]
        return moved

    def send(self, held, port):
        value, owners = held
        value = lax.ppermute(value, ("rep", "slab", "pix"), self.pairs(port))
        return value, [self.move(owner, port) for owner in owners]

    def both(self, held):
        other = self.send(held, "core")
        return other, (jnp.concatenate([held[0], other[0]], axis=0), held[1] + other[1])


def gather_pieces(samples, orient, ports):
    own = (samples, [ports.ids])
    core_own, chip_own = ports.both(own)
    up1 = ports.send(own, "z")
    side0 = ports.send(chip_own, "x|y")
    down = ports.send(own, "back")
    across = ports.send(own, "xy")
    orient = (orient, [ports.ids])
    orient_x = ports.send(orient, "x")
    core_up1, chip_up1 = ports.both(up1)
    up2 = ports.send(up1, "z")
    side1 = ports.send(chip_up1, "x|y")
    orient = (jnp.concatenate([orient[0], orient_x[0]]), orient[1] + orient_x[1])
    orient_core = ports.send(orient, "core")
    orient = (jnp.concatenate([orient[0], orient_core[0]]), orient[1] + orient_core[1])
    core_down, chip_down = ports.both(down)
    across1 = ports.send(across, "z")
    side3 = ports.send(chip_down, "x|y")
    across3 = ports.send(across, "back")
    core_up2, chip_up2 = ports.both(up2)
    side2 = ports.send(chip_up2, "x|y")
    across2 = ports.send(across1, "z")
    pieces = [own, core_own, up1, core_up1, up2, core_up2, down, core_down]
    late = (across, side0, side1, across1, side3, across3, side2, across2)
    for held in late:
        pieces += [held, ports.send(held, "core")]
    owners = np.stack([owner for _, owned in pieces for owner in owned], axis=-1)
    assert (np.sort(owners, -1) == np.arange(ports.ids.size)).all()
    return [value for value, _ in pieces], owners, orient[0], np.stack(orient[1], axis=-1)


def lookup(orient, angle_table):
    choose = (orient[:, None] == lax.iota(jnp.int32, angle_table.shape[0])[None, :]).astype(jnp.int32)
    return jnp.sum(choose[:, :, None, None] * angle_table[None], axis=1)


def corner(indices, lower, fraction):
    return jnp.where(indices == lower, 1.0 - fraction, 0.0) + jnp.where(indices == lower + 1, fraction, 0.0)


def shift_of(size):
    assert size & (size - 1) == 0
    return size.bit_length() - 1


def make_plan(orient, place, table, pieces_n, sizes):
    batch, planes, columns, count_x, row_block, batches = sizes
    items = batch * planes // GROUP
    segments = pieces_n * items
    steps, lane_groups = count_x // row_block, LANES // GROUP
    bits_at = 2 * segments
    info_size = segments + segments * GROUP // TILE + 1
    total_n = batch * batches

    def kernel(orient_ref, place_ref, table_ref, info_ref, where_ref, raw, geometry, found, found_s, listed, sems):
        me = (lax.axis_index("rep") * lax.axis_size("slab") + lax.axis_index("slab")) * lax.axis_size("pix")
        me += lax.axis_index("pix")
        rep, pix = lax.axis_index("rep"), lax.axis_index("pix")
        first_x = (rep * lax.axis_size("pix") + pix) * count_x
        first_z = lax.axis_index("slab") * planes
        copies = [
            pltpu.make_async_copy(table_ref.at[orient_ref[n]], raw.at[place_ref[me, n]], sems.at[n])
            for n in range(total_n)
        ]
        for copy in copies:
            copy.start()
        for copy in copies:
            copy.wait()
        unit = lax.broadcasted_iota(jnp.int32, (1, 4, columns), 1) & 1
        geometry[:, 0:4, :] = raw[...].astype(jnp.float32) * jnp.where(unit == 1, 1.0 / 256.0, 1.0)
        near_x = geometry[:, 0, :] - first_x.astype(jnp.float32)
        near_z = geometry[:, 2, :] - first_z.astype(jnp.float32)
        hit_z = (near_z >= -1.0) & (near_z < planes)
        hits = [
            jnp.where(hit_z & (near_x >= s * row_block - 1.0) & (near_x < (s + 1) * row_block), 1.0, 0.0)
            for s in range(steps)
        ]
        hits = jnp.concatenate(hits, axis=0).astype(jnp.bfloat16)
        lane = lax.broadcasted_iota(jnp.int32, (columns, LANES), 0)
        group = lax.broadcasted_iota(jnp.int32, (columns, LANES), 1)
        member = (lane // GROUP == group).astype(jnp.bfloat16)
        counted = jnp.dot(hits, member, preferred_element_type=jnp.float32)
        bits = jnp.zeros((total_n, LANES), jnp.float32)
        for s in range(steps):
            bits += jnp.where(counted[s * total_n : (s + 1) * total_n] > 0.0, float(2**s), 0.0)
        any_hit = jnp.where(bits > 0.0, 1.0, 0.0).astype(jnp.bfloat16)
        row = lax.broadcasted_iota(jnp.int32, (total_n, total_n), 0)
        col = lax.broadcasted_iota(jnp.int32, (total_n, total_n), 1)
        above = jnp.dot((col < row).astype(jnp.bfloat16), any_hit, preferred_element_type=jnp.float32)
        whole = jnp.dot(jnp.ones((total_n, total_n), jnp.bfloat16), any_hit, preferred_element_type=jnp.float32)
        row = lax.broadcasted_iota(jnp.int32, (LANES, LANES), 0)
        col = lax.broadcasted_iota(jnp.int32, (LANES, LANES), 1)
        before = jnp.dot(
            whole.astype(jnp.bfloat16), (row < col).astype(jnp.bfloat16), preferred_element_type=jnp.float32
        )
        code = jnp.where(bits > 0.0, bits * bits_at + above + before, 0.0)
        found[...] = code.astype(jnp.int32)
        to_scalar = pltpu.make_async_copy(found, found_s, sems.at[0])
        to_scalar.start()
        to_scalar.wait()

        for tile in range(segments, info_size):
            info_ref[tile] = 0

        count = jnp.int32(0)
        for piece in range(pieces_n):
            first_n = place_ref[me, total_n + 2 * piece]
            first_g = place_ref[me, total_n + 2 * piece + 1]
            for item in range(items):
                n, g = first_n + item // (items // batch), first_g + item % (items // batch)
                code = found_s[n, g]
                hit = code > 0
                listed[jnp.where(hit, code & (bits_at - 1), segments)] = n * LANES + g
                info_ref[piece * items + item] = jnp.where(hit, code & (bits_at - 1), segments)
                count += hit.astype(jnp.int32)
        info_ref[info_size - 1] = count
        tiles = (count + TILE // GROUP - 1) >> shift_of(TILE // GROUP)
        lane_group = lax.broadcasted_iota(jnp.int32, (8, LANES), 1) >> shift_of(GROUP)

        def order(block, carry):
            gathered = jnp.full((8, LANES), -4.0, jnp.float32)
            tile_bits = jnp.int32(0)
            for slot in range(lane_groups):
                index = block * lane_groups + slot
                valid = index < count
                name = listed[jnp.minimum(index, count - 1)]
                n, g = name >> shift_of(LANES), name & (LANES - 1)
                tile_bits |= found_s[n, g] >> shift_of(bits_at)
                lanes = pl.ds(pl.multiple_of((g >> shift_of(lane_groups)) * LANES, LANES), LANES)
                shift = ((slot - g) & (lane_groups - 1)) * GROUP
                rolled = pltpu.roll(geometry[n, :, lanes], shift, 1)
                gathered = jnp.where((lane_group == slot) & valid, rolled, gathered)
            where_ref[:, pl.ds(pl.multiple_of(block * LANES, LANES), LANES)] = gathered
            tile = segments + (block >> shift_of(TILE // LANES))
            info_ref[tile] = info_ref[tile] | tile_bits
            return carry

        lax.fori_loop(0, tiles * (TILE // LANES), order, 0)

    smem, vmem = pl.BlockSpec(memory_space=pltpu.SMEM), pl.BlockSpec(memory_space=pltpu.VMEM)
    return pl.pallas_call(
        kernel,
        out_shape=[
            jax.ShapeDtypeStruct((info_size,), jnp.int32),
            jax.ShapeDtypeStruct((8, segments * GROUP), jnp.float32),
        ],
        in_specs=[smem, smem, pl.BlockSpec(memory_space=pl.ANY)],
        out_specs=[smem, vmem],
        scratch_shapes=[
            pltpu.VMEM((total_n, 4, columns), jnp.int32),
            pltpu.VMEM((total_n, 8, columns), jnp.float32),
            pltpu.VMEM((total_n, LANES), jnp.int32),
            pltpu.SMEM((total_n, LANES), jnp.int32),
            pltpu.SMEM((segments + 1,), jnp.int32),
            pltpu.SemaphoreType.DMA((total_n,)),
        ],
        compiler_params=pltpu.CompilerParams(vmem_limit_bytes=4 << 20),
        name="plan",
    )(orient, place, table)


def spread(pieces, info, where, sizes):
    batch, planes, columns, count_x, row_block, _ = sizes
    pieces_n = len(pieces)
    segments = sum(piece.shape[0] for piece in pieces) // GROUP
    steps = count_x // row_block
    channels = 3 * columns

    def kernel(*refs):
        info_ref, where_ref = refs[:2]
        piece_refs = refs[2 : 2 + pieces_n]
        out_ref = refs[2 + pieces_n]
        compact, total, staged, sems = refs[3 + pieces_n :]
        first_x = (lax.axis_index("rep") * lax.axis_size("pix") + lax.axis_index("pix")) * count_x
        first_z = lax.axis_index("slab") * planes
        count = info_ref[segments + segments * GROUP // TILE]
        tiles = (count + TILE // GROUP - 1) >> shift_of(TILE // GROUP)

        first = 0
        for piece in piece_refs:
            items = batch * planes // GROUP
            for start in range(0, piece.shape[0] // GROUP, items):
                targets = [info_ref[first + item] for item in range(items)]
                least = targets[0]
                for target in targets[1:]:
                    least = jnp.minimum(least, target)

                @pl.when(least < segments)
                def _(targets=targets, piece=piece, start=start):
                    for item, target in enumerate(targets):
                        rows = pl.ds(pl.multiple_of(target * GROUP, GROUP), GROUP)
                        source = (start + item) * GROUP
                        compact[rows, :] = piece[source : source + GROUP, :]

                first += items

        def clear(item, carry):
            target = pl.ds(pl.multiple_of(item * GROUP, GROUP), GROUP)
            compact[target, :] = jnp.zeros((GROUP, channels), jnp.bfloat16)
            return carry

        lax.fori_loop(count, tiles * (TILE // GROUP), clear, 0)

        def out_copy(step, slot):
            rows = pl.ds(step * row_block, row_block)
            return pltpu.make_async_copy(staged.at[slot], out_ref.at[rows], sems.at[slot])

        for step in range(steps):
            slot = step % 2

            def product(tile, step=step):
                lanes = pl.ds(pl.multiple_of(tile * TILE, TILE), TILE)
                lower_x, part_x = where_ref[0:1, lanes], where_ref[1:2, lanes]
                lower_z, part_z = where_ref[2:3, lanes], where_ref[3:4, lanes]
                at_x = first_x + step * row_block + lax.broadcasted_iota(jnp.int32, (row_block, TILE), 0)
                at_z = first_z + lax.broadcasted_iota(jnp.int32, (planes, TILE), 0)
                weight_x = corner(at_x.astype(jnp.float32), lower_x, part_x)
                weight_z = corner(at_z.astype(jnp.float32), lower_z, part_z)
                matrix = (weight_x[:, None, :] * weight_z[None, :, :]).astype(jnp.bfloat16)
                matrix = matrix.reshape(row_block * planes, TILE)
                return jnp.dot(matrix, compact[lanes, :], preferred_element_type=jnp.float32)

            def add(tile, seen, step=step, product=product):
                hit = (info_ref[segments + tile] >> step) & 1

                @pl.when((hit > 0) & (seen == 0))
                def _():
                    total[...] = product(tile)

                @pl.when((hit > 0) & (seen > 0))
                def _():
                    total[...] += product(tile)

                return seen + hit

            seen = lax.fori_loop(0, tiles, add, jnp.int32(0))
            if step >= 2:
                out_copy(step - 2, slot).wait()
            shape = (row_block, planes, columns)

            @pl.when(seen > 0)
            def _(slot=slot):
                scale = 1.0 / (total[:, 2 * columns :] + 1.0)
                staged[slot, :, :, :columns] = (total[:, :columns] * scale).reshape(shape)
                staged[slot, :, :, columns:] = (total[:, columns : 2 * columns] * scale).reshape(shape)

            @pl.when(seen == 0)
            def _(slot=slot):
                staged[slot] = jnp.zeros((row_block, planes, 2 * columns), jnp.float32)

            out_copy(step, slot).start()
        for step in range(max(steps - 2, 0), steps):
            out_copy(step, step % 2).wait()

    smem, vmem = pl.BlockSpec(memory_space=pltpu.SMEM), pl.BlockSpec(memory_space=pltpu.VMEM)
    return pl.pallas_call(
        kernel,
        out_shape=jax.ShapeDtypeStruct((count_x, planes, 2 * columns), jnp.float32),
        in_specs=[smem, vmem] + [vmem] * pieces_n,
        out_specs=pl.BlockSpec(memory_space=pl.ANY),
        scratch_shapes=[
            pltpu.VMEM((segments * GROUP + GROUP, channels), jnp.bfloat16),
            pltpu.VMEM((row_block * planes, channels), jnp.float32),
            pltpu.VMEM((2, row_block, planes, 2 * columns), jnp.float32),
            pltpu.SemaphoreType.DMA((2,)),
        ],
        compiler_params=pltpu.CompilerParams(vmem_limit_bytes=14 << 20),
        name="spread",
    )(info, where, *pieces)


def make_body(ports):
    def body(projections, ctf_weight, orient, angle_table):
        batch, planes = projections.shape[:2]
        columns = projections.shape[2] // 2
        count_x = columns // (ports.rep * ports.pix)
        row_block = TILE // planes
        sizes = (batch, planes, columns, count_x, row_block, ports.rep * ports.pix)
        samples = jnp.concatenate([projections, ctf_weight], axis=2).reshape(batch * planes, 3 * columns)
        pieces, owners, orient, orient_owners = gather_pieces(samples, orient, ports)
        place = []
        for owner in (orient_owners, owners):
            rep, slab, pix = np.unravel_index(owner, ports.ids.shape)
            place.append(((rep * ports.pix + pix) * batch, slab * (planes // GROUP)))
        (order, _), (first_n, first_g) = place
        order = order[..., None] + np.arange(batch)
        place = [order.reshape(ports.ids.size, -1), np.stack([first_n, first_g], -1).reshape(ports.ids.size, -1)]
        place = jnp.asarray(np.concatenate(place, axis=1), jnp.int32)
        info, where = make_plan(orient, place, angle_table, owners.shape[-1], sizes)
        return spread(pieces, info, where, sizes)

    return body


def plain_body(projections, ctf_weight, orient, angle_table):
    planes = projections.shape[1]
    columns = projections.shape[2] // 2
    owned_rows = columns // (lax.axis_size("rep") * lax.axis_size("pix"))
    first_z = lax.axis_index("slab") * planes
    first_x = (lax.axis_index("rep") * lax.axis_size("pix") + lax.axis_index("pix")) * owned_rows
    samples = jnp.concatenate([projections, ctf_weight], axis=2)
    samples = lax.all_gather(samples, "slab", axis=1, tiled=True)
    samples = lax.all_gather(samples, BATCH_AXES, axis=0, tiled=True)
    geometry = lookup(lax.all_gather(orient, BATCH_AXES, axis=0, tiled=True), angle_table)
    geometry = geometry.astype(jnp.float32)
    at_x = (first_x + lax.iota(jnp.int32, owned_rows)).astype(jnp.float32)[:, None, None]
    at_z = (first_z + lax.iota(jnp.int32, planes)).astype(jnp.float32)[:, None, None]
    weight_x = corner(at_x, geometry[None, :, 0], geometry[None, :, 1] / 256.0)
    weight_z = corner(at_z, geometry[None, :, 2], geometry[None, :, 3] / 256.0)
    matrix = (weight_x[:, None] * weight_z[None]).astype(jnp.bfloat16).reshape(owned_rows * planes, -1)
    volume = jnp.dot(matrix, samples.reshape(-1, 3 * columns), preferred_element_type=jnp.float32)
    values = volume[:, : 2 * columns].reshape(-1, 2, columns) / (volume[:, None, 2 * columns :] + 1.0)
    return values.reshape(owned_rows, planes, 2 * columns)


def solution(mesh):
    placed = (
        P(BATCH_AXES, "slab", None),
        P(BATCH_AXES, "slab", None),
        P(BATCH_AXES),
        P(),
    )
    ports = Ports(mesh)

    def shard(body):
        return jax.shard_map(
            body, mesh=mesh, in_specs=placed, out_specs=P(BATCH_AXES, "slab", None), check_vma=False
        )

    if not ports.fits():
        return shard(plain_body)
    return shard(make_body(ports))
```

```python
import jax
import jax.numpy as jnp
import numpy as np
from jax import lax
from jax.experimental import pallas as pl
from jax.experimental.pallas import tpu as pltpu
from jax.sharding import PartitionSpec as P


BATCH_AXES = ("rep", "pix")
GROUP = 16
TILE = 256
LANES = 128


class Ports:
    def __init__(self, mesh):
        self.rep, self.slab, self.pix = (mesh.shape[a] for a in ("rep", "slab", "pix"))
        self.ids = np.arange(self.rep * self.slab * self.pix).reshape(self.rep, self.slab, self.pix)

    def fits(self):
        return (self.rep, self.slab, self.pix) == (2, 8, 2)

    def target(self, port, rep, slab, pix):
        if port == "x|y":
            port = "y" if pix else "x"
        if port in ("x", "xy"):
            rep = 1 - rep
        if port in ("y", "xy"):
            slab = slab ^ 1
        if port == "z":
            slab = (slab + 2) % self.slab
        if port == "back":
            slab = (slab - 2) % self.slab
        if port == "core":
            pix = 1 - pix
        return self.ids[rep, slab, pix]

    def pairs(self, port):
        return [(int(self.ids[at]), int(self.target(port, *at))) for at in np.ndindex(self.ids.shape)]

    def move(self, owner, port):
        moved = np.empty_like(owner)
        for source, target in self.pairs(port):
            moved.flat[target] = owner.flat[source]
        return moved

    def send(self, held, port):
        value, owners = held
        value = lax.ppermute(value, ("rep", "slab", "pix"), self.pairs(port))
        return value, [self.move(owner, port) for owner in owners]

    def both(self, held):
        other = self.send(held, "core")
        return other, (jnp.concatenate([held[0], other[0]], axis=0), held[1] + other[1])


def gather_pieces(samples, orient, ports):
    own = (samples, [ports.ids])
    core_own, chip_own = ports.both(own)
    up1 = ports.send(own, "z")
    side0 = ports.send(chip_own, "x|y")
    down = ports.send(own, "back")
    across = ports.send(own, "xy")
    orients = [(orient, [ports.ids])]
    orients.append(ports.send(orients[0], "core"))
    orients += [ports.send(orients[0], "x"), ports.send(orients[1], "x")]
    core_up1, chip_up1 = ports.both(up1)
    up2 = ports.send(up1, "z")
    side1 = ports.send(chip_up1, "x|y")
    core_down, chip_down = ports.both(down)
    across1 = ports.send(across, "z")
    side3 = ports.send(chip_down, "x|y")
    across3 = ports.send(across, "back")
    core_up2, chip_up2 = ports.both(up2)
    side2 = ports.send(chip_up2, "x|y")
    across2 = ports.send(across1, "z")
    pieces = [own, core_own, up1, core_up1, up2, core_up2, down, core_down]
    late = (across, side0, side1, across1, side3, across3, side2, across2)
    for held in late:
        pieces += [held, ports.send(held, "core")]
    owners = np.stack([owner for _, owned in pieces for owner in owned], axis=-1)
    assert (np.sort(owners, -1) == np.arange(ports.ids.size)).all()
    orient_owners = np.stack([owner for _, owned in orients for owner in owned], axis=-1)
    return [value for value, _ in pieces], owners, [value for value, _ in orients], orient_owners


def lookup(orient, angle_table):
    choose = (orient[:, None] == lax.iota(jnp.int32, angle_table.shape[0])[None, :]).astype(jnp.int32)
    return jnp.sum(choose[:, :, None, None] * angle_table[None], axis=1)


def corner(indices, lower, fraction):
    return jnp.where(indices == lower, 1.0 - fraction, 0.0) + jnp.where(indices == lower + 1, fraction, 0.0)


def shift_of(size):
    assert size & (size - 1) == 0
    return size.bit_length() - 1


def make_plan(orients, place, table, pieces_n, sizes):
    batch, planes, columns, count_x, row_block, batches = sizes
    parts = len(orients)
    items = batch * planes // GROUP
    segments = pieces_n * items
    steps, lane_groups = count_x // row_block, LANES // GROUP
    bits_at = 2 * segments
    info_size = segments + segments * GROUP // TILE + 1
    total_n = batch * batches

    def kernel(*refs):
        orient_refs = refs[:parts]
        place_all, table_ref, info_ref, where_ref, place_ref, raw, geometry, found, found_s, listed, sems = refs[parts:]
        me = (lax.axis_index("rep") * lax.axis_size("slab") + lax.axis_index("slab")) * lax.axis_size("pix")
        me += lax.axis_index("pix")
        rep, pix = lax.axis_index("rep"), lax.axis_index("pix")
        first_x = (rep * lax.axis_size("pix") + pix) * count_x
        first_z = lax.axis_index("slab") * planes
        placing = pltpu.make_async_copy(place_all.at[me, 0], place_ref, sems.at[total_n])
        placing.start()
        copies = [
            pltpu.make_async_copy(
                table_ref.at[orient_refs[n // batch][n % batch]], raw.at[n], sems.at[n]
            )
            for n in range(total_n)
        ]
        for copy in copies:
            copy.start()
        placing.wait()
        for copy in copies:
            copy.wait()
        unit = lax.broadcasted_iota(jnp.int32, (1, 4, columns), 1) & 1
        unit = jnp.where(unit[0] == 1, 1.0 / 256.0, 1.0)
        for n in range(total_n):
            geometry[place_ref[n], 0:4, :] = raw[n].astype(jnp.float32) * unit
        near_x = geometry[:, 0, :] - first_x.astype(jnp.float32)
        near_z = geometry[:, 2, :] - first_z.astype(jnp.float32)
        hit_z = (near_z >= -1.0) & (near_z < planes)
        hits = [
            jnp.where(hit_z & (near_x >= s * row_block - 1.0) & (near_x < (s + 1) * row_block), 1.0, 0.0)
            for s in range(steps)
        ]
        hits = jnp.concatenate(hits, axis=0).astype(jnp.bfloat16)
        lane = lax.broadcasted_iota(jnp.int32, (columns, LANES), 0)
        group = lax.broadcasted_iota(jnp.int32, (columns, LANES), 1)
        member = (lane // GROUP == group).astype(jnp.bfloat16)
        counted = jnp.dot(hits, member, preferred_element_type=jnp.float32)
        bits = jnp.zeros((total_n, LANES), jnp.float32)
        for s in range(steps):
            bits += jnp.where(counted[s * total_n : (s + 1) * total_n] > 0.0, float(2**s), 0.0)
        any_hit = jnp.where(bits > 0.0, 1.0, 0.0).astype(jnp.bfloat16)
        row = lax.broadcasted_iota(jnp.int32, (total_n, total_n), 0)
        col = lax.broadcasted_iota(jnp.int32, (total_n, total_n), 1)
        above = jnp.dot((col < row).astype(jnp.bfloat16), any_hit, preferred_element_type=jnp.float32)
        whole = jnp.dot(jnp.ones((total_n, total_n), jnp.bfloat16), any_hit, preferred_element_type=jnp.float32)
        row = lax.broadcasted_iota(jnp.int32, (LANES, LANES), 0)
        col = lax.broadcasted_iota(jnp.int32, (LANES, LANES), 1)
        before = jnp.dot(
            whole.astype(jnp.bfloat16), (row < col).astype(jnp.bfloat16), preferred_element_type=jnp.float32
        )
        code = jnp.where(bits > 0.0, bits * bits_at + above + before, 0.0)
        found[...] = code.astype(jnp.int32)
        to_scalar = pltpu.make_async_copy(found, found_s, sems.at[0])
        to_scalar.start()
        to_scalar.wait()

        for tile in range(segments, info_size):
            info_ref[tile] = 0

        count = jnp.int32(0)
        for piece in range(pieces_n):
            first_n = place_ref[total_n + 2 * piece]
            first_g = place_ref[total_n + 2 * piece + 1]
            for item in range(items):
                n, g = first_n + item // (items // batch), first_g + item % (items // batch)
                code = found_s[n, g]
                hit = code > 0
                listed[jnp.where(hit, code & (bits_at - 1), segments)] = n * LANES + g
                info_ref[piece * items + item] = jnp.where(hit, code & (bits_at - 1), segments)
                count += hit.astype(jnp.int32)
        info_ref[info_size - 1] = count
        tiles = (count + TILE // GROUP - 1) >> shift_of(TILE // GROUP)
        lane_group = lax.broadcasted_iota(jnp.int32, (8, LANES), 1) >> shift_of(GROUP)

        def order(block, carry):
            gathered = jnp.full((8, LANES), -4.0, jnp.float32)
            tile_bits = jnp.int32(0)
            for slot in range(lane_groups):
                index = block * lane_groups + slot
                valid = index < count
                name = listed[jnp.minimum(index, count - 1)]
                n, g = name >> shift_of(LANES), name & (LANES - 1)
                tile_bits |= found_s[n, g] >> shift_of(bits_at)
                lanes = pl.ds(pl.multiple_of((g >> shift_of(lane_groups)) * LANES, LANES), LANES)
                shift = ((slot - g) & (lane_groups - 1)) * GROUP
                rolled = pltpu.roll(geometry[n, :, lanes], shift, 1)
                gathered = jnp.where((lane_group == slot) & valid, rolled, gathered)
            where_ref[:, pl.ds(pl.multiple_of(block * LANES, LANES), LANES)] = gathered
            tile = segments + (block >> shift_of(TILE // LANES))
            info_ref[tile] = info_ref[tile] | tile_bits
            return carry

        lax.fori_loop(0, tiles * (TILE // LANES), order, 0)

    smem, vmem = pl.BlockSpec(memory_space=pltpu.SMEM), pl.BlockSpec(memory_space=pltpu.VMEM)
    return pl.pallas_call(
        kernel,
        out_shape=[
            jax.ShapeDtypeStruct((info_size,), jnp.int32),
            jax.ShapeDtypeStruct((8, segments * GROUP), jnp.float32),
        ],
        in_specs=[smem] * parts + [pl.BlockSpec(memory_space=pltpu.HBM)] * 2,
        out_specs=[smem, vmem],
        scratch_shapes=[
            pltpu.SMEM(place.shape[2:], jnp.int32),
            pltpu.VMEM((total_n, 4, columns), jnp.int32),
            pltpu.VMEM((total_n, 8, columns), jnp.float32),
            pltpu.VMEM((total_n, LANES), jnp.int32),
            pltpu.SMEM((total_n, LANES), jnp.int32),
            pltpu.SMEM((segments + 1,), jnp.int32),
            pltpu.SemaphoreType.DMA((total_n + 1,)),
        ],
        compiler_params=pltpu.CompilerParams(vmem_limit_bytes=4 << 20),
        name="plan",
    )(*orients, place, table)


def spread(pieces, info, where, sizes):
    batch, planes, columns, count_x, row_block, _ = sizes
    pieces_n = len(pieces)
    segments = sum(piece.shape[0] for piece in pieces) // GROUP
    steps = count_x // row_block
    channels = 3 * columns

    def kernel(*refs):
        info_ref, where_ref = refs[:2]
        piece_refs = refs[2 : 2 + pieces_n]
        out_ref = refs[2 + pieces_n]
        compact, total, staged, sems = refs[3 + pieces_n :]
        first_x = (lax.axis_index("rep") * lax.axis_size("pix") + lax.axis_index("pix")) * count_x
        first_z = lax.axis_index("slab") * planes
        count = info_ref[segments + segments * GROUP // TILE]
        tiles = (count + TILE // GROUP - 1) >> shift_of(TILE // GROUP)

        first = 0
        for piece in piece_refs:
            items = batch * planes // GROUP
            for start in range(0, piece.shape[0] // GROUP, items):
                targets = [info_ref[first + item] for item in range(items)]
                least = targets[0]
                for target in targets[1:]:
                    least = jnp.minimum(least, target)

                @pl.when(least < segments)
                def _(targets=targets, piece=piece, start=start):
                    for item, target in enumerate(targets):
                        rows = pl.ds(pl.multiple_of(target * GROUP, GROUP), GROUP)
                        source = (start + item) * GROUP
                        compact[rows, :] = piece[source : source + GROUP, :]

                first += items

        def clear(item, carry):
            target = pl.ds(pl.multiple_of(item * GROUP, GROUP), GROUP)
            compact[target, :] = jnp.zeros((GROUP, channels), jnp.bfloat16)
            return carry

        lax.fori_loop(count, tiles * (TILE // GROUP), clear, 0)

        def out_copy(step, slot):
            rows = pl.ds(step * row_block, row_block)
            return pltpu.make_async_copy(staged.at[slot], out_ref.at[rows], sems.at[slot])

        for step in range(steps):
            slot = step % 2

            def product(tile, step=step):
                lanes = pl.ds(pl.multiple_of(tile * TILE, TILE), TILE)
                lower_x, part_x = where_ref[0:1, lanes], where_ref[1:2, lanes]
                lower_z, part_z = where_ref[2:3, lanes], where_ref[3:4, lanes]
                at_x = first_x + step * row_block + lax.broadcasted_iota(jnp.int32, (row_block, TILE), 0)
                at_z = first_z + lax.broadcasted_iota(jnp.int32, (planes, TILE), 0)
                weight_x = corner(at_x.astype(jnp.float32), lower_x, part_x)
                weight_z = corner(at_z.astype(jnp.float32), lower_z, part_z)
                matrix = (weight_x[:, None, :] * weight_z[None, :, :]).astype(jnp.bfloat16)
                matrix = matrix.reshape(row_block * planes, TILE)
                return jnp.dot(matrix, compact[lanes, :], preferred_element_type=jnp.float32)

            def add(tile, seen, step=step, product=product):
                hit = (info_ref[segments + tile] >> step) & 1

                @pl.when((hit > 0) & (seen == 0))
                def _():
                    total[...] = product(tile)

                @pl.when((hit > 0) & (seen > 0))
                def _():
                    total[...] += product(tile)

                return seen + hit

            seen = lax.fori_loop(0, tiles, add, jnp.int32(0))
            if step >= 2:
                out_copy(step - 2, slot).wait()
            shape = (row_block, planes, columns)

            @pl.when(seen > 0)
            def _(slot=slot):
                scale = 1.0 / (total[:, 2 * columns :] + 1.0)
                staged[slot, :, :, :columns] = (total[:, :columns] * scale).reshape(shape)
                staged[slot, :, :, columns:] = (total[:, columns : 2 * columns] * scale).reshape(shape)

            @pl.when(seen == 0)
            def _(slot=slot):
                staged[slot] = jnp.zeros((row_block, planes, 2 * columns), jnp.float32)

            out_copy(step, slot).start()
        for step in range(max(steps - 2, 0), steps):
            out_copy(step, step % 2).wait()

    smem, vmem = pl.BlockSpec(memory_space=pltpu.SMEM), pl.BlockSpec(memory_space=pltpu.VMEM)
    return pl.pallas_call(
        kernel,
        out_shape=jax.ShapeDtypeStruct((count_x, planes, 2 * columns), jnp.float32),
        in_specs=[smem, vmem] + [vmem] * pieces_n,
        out_specs=pl.BlockSpec(memory_space=pl.ANY),
        scratch_shapes=[
            pltpu.VMEM((segments * GROUP + GROUP, channels), jnp.bfloat16),
            pltpu.VMEM((row_block * planes, channels), jnp.float32),
            pltpu.VMEM((2, row_block, planes, 2 * columns), jnp.float32),
            pltpu.SemaphoreType.DMA((2,)),
        ],
        compiler_params=pltpu.CompilerParams(vmem_limit_bytes=14 << 20),
        name="spread",
    )(info, where, *pieces)


def make_body(ports):
    def body(projections, ctf_weight, orient, angle_table):
        batch, planes = projections.shape[:2]
        columns = projections.shape[2] // 2
        count_x = columns // (ports.rep * ports.pix)
        row_block = TILE // planes
        sizes = (batch, planes, columns, count_x, row_block, ports.rep * ports.pix)
        samples = jnp.concatenate([projections, ctf_weight], axis=2).reshape(batch * planes, 3 * columns)
        pieces, owners, orients, orient_owners = gather_pieces(samples, orient, ports)
        place = []
        for owner in (orient_owners, owners):
            rep, slab, pix = np.unravel_index(owner, ports.ids.shape)
            place.append(((rep * ports.pix + pix) * batch, slab * (planes // GROUP)))
        (order, _), (first_n, first_g) = place
        order = order[..., None] + np.arange(batch)
        place = [order.reshape(ports.ids.size, -1), np.stack([first_n, first_g], -1).reshape(ports.ids.size, -1)]
        place = np.concatenate(place, axis=1)
        place = np.pad(place, ((0, 0), (0, -place.shape[1] % LANES)))[:, None]
        info, where = make_plan(orients, jnp.asarray(place, jnp.int32), angle_table, owners.shape[-1], sizes)
        return spread(pieces, info, where, sizes)

    return body


def plain_body(projections, ctf_weight, orient, angle_table):
    planes = projections.shape[1]
    columns = projections.shape[2] // 2
    owned_rows = columns // (lax.axis_size("rep") * lax.axis_size("pix"))
    first_z = lax.axis_index("slab") * planes
    first_x = (lax.axis_index("rep") * lax.axis_size("pix") + lax.axis_index("pix")) * owned_rows
    samples = jnp.concatenate([projections, ctf_weight], axis=2)
    samples = lax.all_gather(samples, "slab", axis=1, tiled=True)
    samples = lax.all_gather(samples, BATCH_AXES, axis=0, tiled=True)
    geometry = lookup(lax.all_gather(orient, BATCH_AXES, axis=0, tiled=True), angle_table)
    geometry = geometry.astype(jnp.float32)
    at_x = (first_x + lax.iota(jnp.int32, owned_rows)).astype(jnp.float32)[:, None, None]
    at_z = (first_z + lax.iota(jnp.int32, planes)).astype(jnp.float32)[:, None, None]
    weight_x = corner(at_x, geometry[None, :, 0], geometry[None, :, 1] / 256.0)
    weight_z = corner(at_z, geometry[None, :, 2], geometry[None, :, 3] / 256.0)
    matrix = (weight_x[:, None] * weight_z[None]).astype(jnp.bfloat16).reshape(owned_rows * planes, -1)
    volume = jnp.dot(matrix, samples.reshape(-1, 3 * columns), preferred_element_type=jnp.float32)
    values = volume[:, : 2 * columns].reshape(-1, 2, columns) / (volume[:, None, 2 * columns :] + 1.0)
    return values.reshape(owned_rows, planes, 2 * columns)


def solution(mesh):
    placed = (
        P(BATCH_AXES, "slab", None),
        P(BATCH_AXES, "slab", None),
        P(BATCH_AXES),
        P(),
    )
    ports = Ports(mesh)

    def shard(body):
        return jax.shard_map(
            body, mesh=mesh, in_specs=placed, out_specs=P(BATCH_AXES, "slab", None), check_vma=False
        )

    if not ports.fits():
        return shard(plain_body)
    return shard(make_body(ports))
```

```python
import jax
import jax.numpy as jnp
import numpy as np
from jax import lax
from jax.experimental import pallas as pl
from jax.experimental.pallas import tpu as pltpu
from jax.sharding import PartitionSpec as P


BATCH_AXES = ("rep", "pix")
GROUP = 16
TILE = 256
LANES = 128


class Ports:
    def __init__(self, mesh):
        self.rep, self.slab, self.pix = (mesh.shape[a] for a in ("rep", "slab", "pix"))
        self.ids = np.arange(self.rep * self.slab * self.pix).reshape(self.rep, self.slab, self.pix)

    def fits(self):
        return (self.rep, self.slab, self.pix) == (2, 8, 2)

    def target(self, port, rep, slab, pix):
        if "|" in port:
            port = port.split("|")[pix]
        if port in ("x", "xy"):
            rep = 1 - rep
        if port in ("y", "xy"):
            slab = slab ^ 1
        if port == "z":
            slab = (slab + 2) % self.slab
        if port == "back":
            slab = (slab - 2) % self.slab
        if port == "core":
            pix = 1 - pix
        return self.ids[rep, slab, pix]

    def pairs(self, port):
        return [(int(self.ids[at]), int(self.target(port, *at))) for at in np.ndindex(self.ids.shape)]

    def move(self, owner, port):
        moved = np.empty_like(owner)
        for source, target in self.pairs(port):
            moved.flat[target] = owner.flat[source]
        return moved

    def send(self, held, port):
        value, owners = held
        value = lax.ppermute(value, ("rep", "slab", "pix"), self.pairs(port))
        return value, [self.move(owner, port) for owner in owners]

    def distances(self, owners):
        found = []
        for piece in range(owners.shape[-1]):
            per_core = []
            for pix in range(self.pix):
                rep, slab, core = np.unravel_index(owners[0, 0, pix, piece], self.ids.shape)
                per_core.append((int(rep), int(slab // 2), int(slab % 2), int(core) ^ pix))
            for at in np.ndindex(self.ids.shape):
                rep, slab, core = self.owner(per_core[at[2]], *at)
                assert self.ids[rep, slab, core] == owners[at][piece]
            found.append(per_core)
        return found

    def owner(self, distance, rep, slab, pix):
        far_x, far_z, far_y, far_core = distance
        upper = (slab // 2 + far_z) & (self.slab // 2 - 1)
        return rep ^ far_x, upper * 2 + ((slab & 1) ^ far_y), pix ^ far_core

    def both(self, held):
        other = self.send(held, "core")
        return other, (jnp.concatenate([held[0], other[0]], axis=0), held[1] + other[1])


def gather_pieces(samples, orient, ports):
    own = (samples, [ports.ids])
    core_own, chip_own = ports.both(own)
    up1 = ports.send(own, "z")
    side0 = ports.send(chip_own, "x|y")
    down = ports.send(own, "back")
    across = ports.send(own, "xy")
    orients = [(orient, [ports.ids])]
    orients.append(ports.send(orients[0], "core"))
    orients += [ports.send(orients[0], "x")]
    orients.append(ports.send(orients[2], "core"))
    core_up1, chip_up1 = ports.both(up1)
    up2 = ports.send(up1, "z")
    side1 = ports.send(chip_up1, "x|y")
    core_down, chip_down = ports.both(down)
    across1 = ports.send(across, "z")
    side3 = ports.send(chip_down, "x|y")
    across3 = ports.send(across, "back")
    core_up2, chip_up2 = ports.both(up2)
    side2 = ports.send(chip_up2, "x|y")
    across2 = ports.send(up2, "xy")
    pieces = [own, core_own, up1, core_up1, up2, core_up2, down, core_down]
    late = (across, side0, side1, across1, side3, across3, side2, across2)
    for held in late:
        pieces += [held, ports.send(held, "core")]
    owners = np.stack([owner for _, owned in pieces for owner in owned], axis=-1)
    assert (np.sort(owners, -1) == np.arange(ports.ids.size)).all()
    orient_owners = np.stack([owner for _, owned in orients for owner in owned], axis=-1)
    return [value for value, _ in pieces], owners, [value for value, _ in orients], orient_owners


def lookup(orient, angle_table):
    choose = (orient[:, None] == lax.iota(jnp.int32, angle_table.shape[0])[None, :]).astype(jnp.int32)
    return jnp.sum(choose[:, :, None, None] * angle_table[None], axis=1)


def corner(indices, lower, fraction):
    return jnp.where(indices == lower, 1.0 - fraction, 0.0) + jnp.where(indices == lower + 1, fraction, 0.0)


def shift_of(size):
    assert size & (size - 1) == 0
    return size.bit_length() - 1


def make_plan(ports, orients, orders, table, distances, sizes):
    batch, planes, columns, count_x, row_block, batches = sizes
    parts, pieces_n = len(orients), len(distances)
    items = batch * planes // GROUP
    segments = pieces_n * items
    steps, lane_groups = count_x // row_block, LANES // GROUP
    bits_at = 2 * segments
    info_size = segments + segments * GROUP // TILE + 1
    total_n = batch * batches

    def kernel(*refs):
        orient_refs = refs[:parts]
        table_ref, info_ref, where_ref, raw, geometry, found, found_s, listed, sems = refs[parts:]
        rep, slab, pix = (lax.axis_index(axis) for axis in ("rep", "slab", "pix"))
        first_x = (rep * ports.pix + pix) * count_x
        first_z = slab * planes
        known = {}

        def place(per_core):
            for distance in per_core:
                if distance not in known:
                    at_rep, at_slab, at_pix = ports.owner(distance, rep, slab, pix)
                    known[distance] = (at_rep * ports.pix + at_pix) * batch, at_slab * (planes // GROUP)
            if len(set(per_core)) == 1:
                return known[per_core[0]]
            return [jnp.where(pix == 0, first, second) for first, second in zip(*(known[d] for d in per_core))]

        copies = [
            pltpu.make_async_copy(
                table_ref.at[orient_refs[n // batch][n % batch]], raw.at[n], sems.at[n]
            )
            for n in range(total_n)
        ]
        for copy in copies:
            copy.start()
        for copy in copies:
            copy.wait()
        unit = lax.broadcasted_iota(jnp.int32, (1, 4, columns), 1) & 1
        unit = jnp.where(unit[0] == 1, 1.0 / 256.0, 1.0)
        for n in range(total_n):
            geometry[place(orders[n // batch])[0] + n % batch, 0:4, :] = raw[n].astype(jnp.float32) * unit
        near_x = geometry[:, 0, :] - first_x.astype(jnp.float32)
        near_z = geometry[:, 2, :] - first_z.astype(jnp.float32)
        hit_z = (near_z >= -1.0) & (near_z < planes)
        hits = [
            jnp.where(hit_z & (near_x >= s * row_block - 1.0) & (near_x < (s + 1) * row_block), 1.0, 0.0)
            for s in range(steps)
        ]
        hits = jnp.concatenate(hits, axis=0).astype(jnp.bfloat16)
        lane = lax.broadcasted_iota(jnp.int32, (columns, LANES), 0)
        group = lax.broadcasted_iota(jnp.int32, (columns, LANES), 1)
        member = (lane // GROUP == group).astype(jnp.bfloat16)
        counted = jnp.dot(hits, member, preferred_element_type=jnp.float32)
        bits = jnp.zeros((total_n, LANES), jnp.float32)
        for s in range(steps):
            bits += jnp.where(counted[s * total_n : (s + 1) * total_n] > 0.0, float(2**s), 0.0)
        any_hit = jnp.where(bits > 0.0, 1.0, 0.0).astype(jnp.bfloat16)
        row = lax.broadcasted_iota(jnp.int32, (total_n, total_n), 0)
        col = lax.broadcasted_iota(jnp.int32, (total_n, total_n), 1)
        above = jnp.dot((col < row).astype(jnp.bfloat16), any_hit, preferred_element_type=jnp.float32)
        whole = jnp.dot(jnp.ones((total_n, total_n), jnp.bfloat16), any_hit, preferred_element_type=jnp.float32)
        row = lax.broadcasted_iota(jnp.int32, (LANES, LANES), 0)
        col = lax.broadcasted_iota(jnp.int32, (LANES, LANES), 1)
        before = jnp.dot(
            whole.astype(jnp.bfloat16), (row < col).astype(jnp.bfloat16), preferred_element_type=jnp.float32
        )
        code = jnp.where(bits > 0.0, bits * bits_at + above + before, 0.0)
        found[...] = code.astype(jnp.int32)
        to_scalar = pltpu.make_async_copy(found, found_s, sems.at[0])
        to_scalar.start()
        to_scalar.wait()

        for tile in range(segments, info_size):
            info_ref[tile] = 0

        count = jnp.int32(0)
        for piece in range(pieces_n):
            first_n, first_g = place(distances[piece])
            for item in range(items):
                n, g = first_n + item // (items // batch), first_g + item % (items // batch)
                code = found_s[n, g]
                hit = code > 0
                listed[jnp.where(hit, code & (bits_at - 1), segments)] = n * LANES + g
                info_ref[piece * items + item] = jnp.where(hit, code & (bits_at - 1), segments)
                count += hit.astype(jnp.int32)
        info_ref[info_size - 1] = count
        tiles = (count + TILE // GROUP - 1) >> shift_of(TILE // GROUP)
        lane_group = lax.broadcasted_iota(jnp.int32, (8, LANES), 1) >> shift_of(GROUP)

        def order(block, carry):
            gathered = jnp.full((8, LANES), -4.0, jnp.float32)
            tile_bits = jnp.int32(0)
            for slot in range(lane_groups):
                index = block * lane_groups + slot
                valid = index < count
                name = listed[jnp.minimum(index, count - 1)]
                n, g = name >> shift_of(LANES), name & (LANES - 1)
                tile_bits |= found_s[n, g] >> shift_of(bits_at)
                lanes = pl.ds(pl.multiple_of((g >> shift_of(lane_groups)) * LANES, LANES), LANES)
                shift = ((slot - g) & (lane_groups - 1)) * GROUP
                rolled = pltpu.roll(geometry[n, :, lanes], shift, 1)
                gathered = jnp.where((lane_group == slot) & valid, rolled, gathered)
            where_ref[:, pl.ds(pl.multiple_of(block * LANES, LANES), LANES)] = gathered
            tile = segments + (block >> shift_of(TILE // LANES))
            info_ref[tile] = info_ref[tile] | tile_bits
            return carry

        lax.fori_loop(0, tiles * (TILE // LANES), order, 0)

    smem, vmem = pl.BlockSpec(memory_space=pltpu.SMEM), pl.BlockSpec(memory_space=pltpu.VMEM)
    return pl.pallas_call(
        kernel,
        out_shape=[
            jax.ShapeDtypeStruct((info_size,), jnp.int32),
            jax.ShapeDtypeStruct((8, segments * GROUP), jnp.float32),
        ],
        in_specs=[smem] * parts + [pl.BlockSpec(memory_space=pl.ANY)],
        out_specs=[smem, vmem],
        scratch_shapes=[
            pltpu.VMEM((total_n, 4, columns), jnp.int32),
            pltpu.VMEM((total_n, 8, columns), jnp.float32),
            pltpu.VMEM((total_n, LANES), jnp.int32),
            pltpu.SMEM((total_n, LANES), jnp.int32),
            pltpu.SMEM((segments + 1,), jnp.int32),
            pltpu.SemaphoreType.DMA((total_n,)),
        ],
        compiler_params=pltpu.CompilerParams(vmem_limit_bytes=4 << 20),
        name="plan",
    )(*orients, table)


def spread(pieces, info, where, sizes):
    batch, planes, columns, count_x, row_block, _ = sizes
    pieces_n = len(pieces)
    segments = sum(piece.shape[0] for piece in pieces) // GROUP
    steps = count_x // row_block
    channels = 3 * columns

    def kernel(*refs):
        info_ref, where_ref = refs[:2]
        piece_refs = refs[2 : 2 + pieces_n]
        out_ref = refs[2 + pieces_n]
        compact, total, staged, sems = refs[3 + pieces_n :]
        first_x = (lax.axis_index("rep") * lax.axis_size("pix") + lax.axis_index("pix")) * count_x
        first_z = lax.axis_index("slab") * planes
        count = info_ref[segments + segments * GROUP // TILE]
        tiles = (count + TILE // GROUP - 1) >> shift_of(TILE // GROUP)

        first = 0
        for piece in piece_refs:
            items = batch * planes // GROUP
            for start in range(0, piece.shape[0] // GROUP, items):
                targets = [info_ref[first + item] for item in range(items)]
                least = targets[0]
                for target in targets[1:]:
                    least = jnp.minimum(least, target)

                @pl.when(least < segments)
                def _(targets=targets, piece=piece, start=start):
                    for item, target in enumerate(targets):
                        rows = pl.ds(pl.multiple_of(target * GROUP, GROUP), GROUP)
                        source = (start + item) * GROUP
                        compact[rows, :] = piece[source : source + GROUP, :]

                first += items

        def clear(item, carry):
            target = pl.ds(pl.multiple_of(item * GROUP, GROUP), GROUP)
            compact[target, :] = jnp.zeros((GROUP, channels), jnp.bfloat16)
            return carry

        lax.fori_loop(count, tiles * (TILE // GROUP), clear, 0)

        def out_copy(step, slot):
            rows = pl.ds(step * row_block, row_block)
            return pltpu.make_async_copy(staged.at[slot], out_ref.at[rows], sems.at[slot])

        for step in range(steps):
            slot = step % 2

            def product(tile, step=step):
                lanes = pl.ds(pl.multiple_of(tile * TILE, TILE), TILE)
                lower_x, part_x = where_ref[0:1, lanes], where_ref[1:2, lanes]
                lower_z, part_z = where_ref[2:3, lanes], where_ref[3:4, lanes]
                at_x = first_x + step * row_block + lax.broadcasted_iota(jnp.int32, (row_block, TILE), 0)
                at_z = first_z + lax.broadcasted_iota(jnp.int32, (planes, TILE), 0)
                weight_x = corner(at_x.astype(jnp.float32), lower_x, part_x)
                weight_z = corner(at_z.astype(jnp.float32), lower_z, part_z)
                matrix = (weight_x[:, None, :] * weight_z[None, :, :]).astype(jnp.bfloat16)
                matrix = matrix.reshape(row_block * planes, TILE)
                return jnp.dot(matrix, compact[lanes, :], preferred_element_type=jnp.float32)

            def add(tile, seen, step=step, product=product):
                hit = (info_ref[segments + tile] >> step) & 1

                @pl.when((hit > 0) & (seen == 0))
                def _():
                    total[...] = product(tile)

                @pl.when((hit > 0) & (seen > 0))
                def _():
                    total[...] += product(tile)

                return seen + hit

            seen = lax.fori_loop(0, tiles, add, jnp.int32(0))
            if step >= 2:
                out_copy(step - 2, slot).wait()
            shape = (row_block, planes, columns)

            @pl.when(seen > 0)
            def _(slot=slot):
                scale = 1.0 / (total[:, 2 * columns :] + 1.0)
                staged[slot, :, :, :columns] = (total[:, :columns] * scale).reshape(shape)
                staged[slot, :, :, columns:] = (total[:, columns : 2 * columns] * scale).reshape(shape)

            @pl.when(seen == 0)
            def _(slot=slot):
                staged[slot] = jnp.zeros((row_block, planes, 2 * columns), jnp.float32)

            out_copy(step, slot).start()
        for step in range(max(steps - 2, 0), steps):
            out_copy(step, step % 2).wait()

    smem, vmem = pl.BlockSpec(memory_space=pltpu.SMEM), pl.BlockSpec(memory_space=pltpu.VMEM)
    return pl.pallas_call(
        kernel,
        out_shape=jax.ShapeDtypeStruct((count_x, planes, 2 * columns), jnp.float32),
        in_specs=[smem, vmem] + [vmem] * pieces_n,
        out_specs=pl.BlockSpec(memory_space=pl.ANY),
        scratch_shapes=[
            pltpu.VMEM((segments * GROUP + GROUP, channels), jnp.bfloat16),
            pltpu.VMEM((row_block * planes, channels), jnp.float32),
            pltpu.VMEM((2, row_block, planes, 2 * columns), jnp.float32),
            pltpu.SemaphoreType.DMA((2,)),
        ],
        compiler_params=pltpu.CompilerParams(vmem_limit_bytes=14 << 20),
        name="spread",
    )(info, where, *pieces)


def make_body(ports):
    def body(projections, ctf_weight, orient, angle_table):
        batch, planes = projections.shape[:2]
        columns = projections.shape[2] // 2
        count_x = columns // (ports.rep * ports.pix)
        row_block = TILE // planes
        sizes = (batch, planes, columns, count_x, row_block, ports.rep * ports.pix)
        samples = jnp.concatenate([projections, ctf_weight], axis=2).reshape(batch * planes, 3 * columns)
        pieces, owners, orients, orient_owners = gather_pieces(samples, orient, ports)
        info, where = make_plan(
            ports, orients, ports.distances(orient_owners), angle_table, ports.distances(owners), sizes
        )
        return spread(pieces, info, where, sizes)

    return body


def plain_body(projections, ctf_weight, orient, angle_table):
    planes = projections.shape[1]
    columns = projections.shape[2] // 2
    owned_rows = columns // (lax.axis_size("rep") * lax.axis_size("pix"))
    first_z = lax.axis_index("slab") * planes
    first_x = (lax.axis_index("rep") * lax.axis_size("pix") + lax.axis_index("pix")) * owned_rows
    samples = jnp.concatenate([projections, ctf_weight], axis=2)
    samples = lax.all_gather(samples, "slab", axis=1, tiled=True)
    samples = lax.all_gather(samples, BATCH_AXES, axis=0, tiled=True)
    geometry = lookup(lax.all_gather(orient, BATCH_AXES, axis=0, tiled=True), angle_table)
    geometry = geometry.astype(jnp.float32)
    at_x = (first_x + lax.iota(jnp.int32, owned_rows)).astype(jnp.float32)[:, None, None]
    at_z = (first_z + lax.iota(jnp.int32, planes)).astype(jnp.float32)[:, None, None]
    weight_x = corner(at_x, geometry[None, :, 0], geometry[None, :, 1] / 256.0)
    weight_z = corner(at_z, geometry[None, :, 2], geometry[None, :, 3] / 256.0)
    matrix = (weight_x[:, None] * weight_z[None]).astype(jnp.bfloat16).reshape(owned_rows * planes, -1)
    volume = jnp.dot(matrix, samples.reshape(-1, 3 * columns), preferred_element_type=jnp.float32)
    values = volume[:, : 2 * columns].reshape(-1, 2, columns) / (volume[:, None, 2 * columns :] + 1.0)
    return values.reshape(owned_rows, planes, 2 * columns)


def solution(mesh):
    placed = (
        P(BATCH_AXES, "slab", None),
        P(BATCH_AXES, "slab", None),
        P(BATCH_AXES),
        P(),
    )
    ports = Ports(mesh)

    def shard(body):
        return jax.shard_map(
            body, mesh=mesh, in_specs=placed, out_specs=P(BATCH_AXES, "slab", None), check_vma=False
        )

    if not ports.fits():
        return shard(plain_body)
    return shard(make_body(ports))
```

```python
import jax
import jax.numpy as jnp
import numpy as np
from jax import lax
from jax.experimental import pallas as pl
from jax.experimental.pallas import tpu as pltpu
from jax.sharding import PartitionSpec as P


BATCH_AXES = ("rep", "pix")
GROUP = 16
TILE = 256
LANES = 128


class Ports:
    def __init__(self, mesh):
        self.rep, self.slab, self.pix = (mesh.shape[a] for a in ("rep", "slab", "pix"))
        self.ids = np.arange(self.rep * self.slab * self.pix).reshape(self.rep, self.slab, self.pix)

    def fits(self):
        return (self.rep, self.slab, self.pix) == (2, 8, 2)

    def target(self, port, rep, slab, pix):
        if "|" in port:
            port = port.split("|")[pix]
        if port in ("x", "xy"):
            rep = 1 - rep
        if port in ("y", "xy"):
            slab = slab ^ 1
        if port == "z":
            slab = (slab + 2) % self.slab
        if port == "back":
            slab = (slab - 2) % self.slab
        if port == "core":
            pix = 1 - pix
        return self.ids[rep, slab, pix]

    def pairs(self, port):
        return [(int(self.ids[at]), int(self.target(port, *at))) for at in np.ndindex(self.ids.shape)]

    def move(self, owner, port):
        moved = np.empty_like(owner)
        for source, target in self.pairs(port):
            moved.flat[target] = owner.flat[source]
        return moved

    def send(self, held, port):
        value, owners = held
        value = lax.ppermute(value, ("rep", "slab", "pix"), self.pairs(port))
        return value, [self.move(owner, port) for owner in owners]

    def distances(self, owners):
        found = []
        for piece in range(owners.shape[-1]):
            per_core = []
            for pix in range(self.pix):
                rep, slab, core = np.unravel_index(owners[0, 0, pix, piece], self.ids.shape)
                per_core.append((int(rep), int(slab // 2), int(slab % 2), int(core) ^ pix))
            for at in np.ndindex(self.ids.shape):
                rep, slab, core = self.owner(per_core[at[2]], *at)
                assert self.ids[rep, slab, core] == owners[at][piece]
            found.append(per_core)
        return found

    def owner(self, distance, rep, slab, pix):
        far_x, far_z, far_y, far_core = distance
        upper = (slab // 2 + far_z) & (self.slab // 2 - 1)
        return rep ^ far_x, upper * 2 + ((slab & 1) ^ far_y), pix ^ far_core

    def both(self, held):
        other = self.send(held, "core")
        return other, (jnp.concatenate([held[0], other[0]], axis=0), held[1] + other[1])


def gather_pieces(samples, orient, ports):
    own = (samples, [ports.ids])
    core_own, chip_own = ports.both(own)
    up1 = ports.send(own, "z")
    side0 = ports.send(chip_own, "x|y")
    down = ports.send(own, "back")
    across = ports.send(own, "xy")
    orients = [(orient, [ports.ids])]
    orients.append(ports.send(orients[0], "core"))
    orients += [ports.send(orients[0], "x")]
    orients.append(ports.send(orients[2], "core"))
    core_up1, chip_up1 = ports.both(up1)
    up2 = ports.send(up1, "z")
    side1 = ports.send(chip_up1, "x|y")
    core_down, chip_down = ports.both(down)
    across1 = ports.send(across, "z")
    side3 = ports.send(chip_down, "x|y")
    across3 = ports.send(across, "back")
    core_up2, chip_up2 = ports.both(up2)
    side2 = ports.send(chip_up2, "x|y")
    across2 = ports.send(up2, "xy")
    pieces = [own, core_own, up1, core_up1, up2, core_up2, down, core_down]
    late = (across, side0, side1, across1, side3, across3, side2, across2)
    for held in late:
        pieces += [held, ports.send(held, "core")]
    owners = np.stack([owner for _, owned in pieces for owner in owned], axis=-1)
    assert (np.sort(owners, -1) == np.arange(ports.ids.size)).all()
    orient_owners = np.stack([owner for _, owned in orients for owner in owned], axis=-1)
    return [value for value, _ in pieces], owners, [value for value, _ in orients], orient_owners


def lookup(orient, angle_table):
    choose = (orient[:, None] == lax.iota(jnp.int32, angle_table.shape[0])[None, :]).astype(jnp.int32)
    return jnp.sum(choose[:, :, None, None] * angle_table[None], axis=1)


def corner(indices, lower, fraction):
    return jnp.where(indices == lower, 1.0 - fraction, 0.0) + jnp.where(indices == lower + 1, fraction, 0.0)


def shift_of(size):
    assert size & (size - 1) == 0
    return size.bit_length() - 1


def make_plan(ports, orients, orders, table, distances, sizes):
    batch, planes, columns, count_x, row_block, batches = sizes
    parts, pieces_n = len(orients), len(distances)
    items = batch * planes // GROUP
    segments = pieces_n * items
    steps, lane_groups = count_x // row_block, LANES // GROUP
    bits_at = 2 * segments
    tiles_max = segments * GROUP // TILE
    counts_at = segments + steps * tiles_max
    info_size = counts_at + steps + 1
    total_n = batch * batches

    def kernel(*refs):
        orient_refs = refs[:parts]
        table_ref, info_ref, where_ref, raw, geometry, found, found_s, listed, touched, sems = refs[parts:]
        rep, slab, pix = (lax.axis_index(axis) for axis in ("rep", "slab", "pix"))
        first_x = (rep * ports.pix + pix) * count_x
        first_z = slab * planes
        known = {}

        def place(per_core):
            for distance in per_core:
                if distance not in known:
                    at_rep, at_slab, at_pix = ports.owner(distance, rep, slab, pix)
                    known[distance] = (at_rep * ports.pix + at_pix) * batch, at_slab * (planes // GROUP)
            if len(set(per_core)) == 1:
                return known[per_core[0]]
            return [jnp.where(pix == 0, first, second) for first, second in zip(*(known[d] for d in per_core))]

        copies = [
            pltpu.make_async_copy(
                table_ref.at[orient_refs[n // batch][n % batch]], raw.at[n], sems.at[n]
            )
            for n in range(total_n)
        ]
        for copy in copies:
            copy.start()
        for copy in copies:
            copy.wait()
        unit = lax.broadcasted_iota(jnp.int32, (1, 4, columns), 1) & 1
        unit = jnp.where(unit[0] == 1, 1.0 / 256.0, 1.0)
        for n in range(total_n):
            geometry[place(orders[n // batch])[0] + n % batch, 0:4, :] = raw[n].astype(jnp.float32) * unit
        near_x = geometry[:, 0, :] - first_x.astype(jnp.float32)
        near_z = geometry[:, 2, :] - first_z.astype(jnp.float32)
        hit_z = (near_z >= -1.0) & (near_z < planes)
        hits = [
            jnp.where(hit_z & (near_x >= s * row_block - 1.0) & (near_x < (s + 1) * row_block), 1.0, 0.0)
            for s in range(steps)
        ]
        hits = jnp.concatenate(hits, axis=0).astype(jnp.bfloat16)
        lane = lax.broadcasted_iota(jnp.int32, (columns, LANES), 0)
        group = lax.broadcasted_iota(jnp.int32, (columns, LANES), 1)
        member = (lane // GROUP == group).astype(jnp.bfloat16)
        counted = jnp.dot(hits, member, preferred_element_type=jnp.float32)
        bits = jnp.zeros((total_n, LANES), jnp.float32)
        for s in range(steps):
            bits += jnp.where(counted[s * total_n : (s + 1) * total_n] > 0.0, float(2**s), 0.0)
        any_hit = jnp.where(bits > 0.0, 1.0, 0.0).astype(jnp.bfloat16)
        row = lax.broadcasted_iota(jnp.int32, (total_n, total_n), 0)
        col = lax.broadcasted_iota(jnp.int32, (total_n, total_n), 1)
        above = jnp.dot((col < row).astype(jnp.bfloat16), any_hit, preferred_element_type=jnp.float32)
        whole = jnp.dot(jnp.ones((total_n, total_n), jnp.bfloat16), any_hit, preferred_element_type=jnp.float32)
        row = lax.broadcasted_iota(jnp.int32, (LANES, LANES), 0)
        col = lax.broadcasted_iota(jnp.int32, (LANES, LANES), 1)
        before = jnp.dot(
            whole.astype(jnp.bfloat16), (row < col).astype(jnp.bfloat16), preferred_element_type=jnp.float32
        )
        code = jnp.where(bits > 0.0, bits * bits_at + above + before, 0.0)
        found[...] = code.astype(jnp.int32)
        to_scalar = pltpu.make_async_copy(found, found_s, sems.at[0])
        to_scalar.start()
        to_scalar.wait()

        for tile in range(tiles_max):
            touched[tile] = 0

        count = jnp.int32(0)
        for piece in range(pieces_n):
            first_n, first_g = place(distances[piece])
            for item in range(items):
                n, g = first_n + item // (items // batch), first_g + item % (items // batch)
                code = found_s[n, g]
                hit = code > 0
                listed[jnp.where(hit, code & (bits_at - 1), segments)] = n * LANES + g
                info_ref[piece * items + item] = jnp.where(hit, code & (bits_at - 1), segments)
                count += hit.astype(jnp.int32)
        info_ref[info_size - 1] = count
        tiles = (count + TILE // GROUP - 1) >> shift_of(TILE // GROUP)
        lane_group = lax.broadcasted_iota(jnp.int32, (8, LANES), 1) >> shift_of(GROUP)

        def order(block, carry):
            gathered = jnp.full((8, LANES), -4.0, jnp.float32)
            tile_bits = jnp.int32(0)
            for slot in range(lane_groups):
                index = block * lane_groups + slot
                valid = index < count
                name = listed[jnp.minimum(index, count - 1)]
                n, g = name >> shift_of(LANES), name & (LANES - 1)
                tile_bits |= found_s[n, g] >> shift_of(bits_at)
                lanes = pl.ds(pl.multiple_of((g >> shift_of(lane_groups)) * LANES, LANES), LANES)
                shift = ((slot - g) & (lane_groups - 1)) * GROUP
                rolled = pltpu.roll(geometry[n, :, lanes], shift, 1)
                gathered = jnp.where((lane_group == slot) & valid, rolled, gathered)
            where_ref[:, pl.ds(pl.multiple_of(block * LANES, LANES), LANES)] = gathered
            tile = block >> shift_of(TILE // LANES)
            touched[tile] = touched[tile] | tile_bits
            return carry

        lax.fori_loop(0, tiles * (TILE // LANES), order, 0)

        def to_steps(tile, counts):
            tile_bits = touched[tile]
            for s in range(steps):
                info_ref[segments + s * tiles_max + counts[s]] = tile
            return tuple(counts[s] + ((tile_bits >> s) & 1) for s in range(steps))

        counts = lax.fori_loop(0, tiles, to_steps, (jnp.int32(0),) * steps)
        for s in range(steps):
            info_ref[counts_at + s] = counts[s]

    smem, vmem = pl.BlockSpec(memory_space=pltpu.SMEM), pl.BlockSpec(memory_space=pltpu.VMEM)
    return pl.pallas_call(
        kernel,
        out_shape=[
            jax.ShapeDtypeStruct((info_size,), jnp.int32),
            jax.ShapeDtypeStruct((8, segments * GROUP), jnp.float32),
        ],
        in_specs=[smem] * parts + [pl.BlockSpec(memory_space=pl.ANY)],
        out_specs=[smem, vmem],
        scratch_shapes=[
            pltpu.VMEM((total_n, 4, columns), jnp.int32),
            pltpu.VMEM((total_n, 8, columns), jnp.float32),
            pltpu.VMEM((total_n, LANES), jnp.int32),
            pltpu.SMEM((total_n, LANES), jnp.int32),
            pltpu.SMEM((segments + 1,), jnp.int32),
            pltpu.SMEM((tiles_max,), jnp.int32),
            pltpu.SemaphoreType.DMA((total_n,)),
        ],
        compiler_params=pltpu.CompilerParams(vmem_limit_bytes=4 << 20),
        name="plan",
    )(*orients, table)


def spread(pieces, info, where, sizes):
    batch, planes, columns, count_x, row_block, _ = sizes
    pieces_n = len(pieces)
    segments = sum(piece.shape[0] for piece in pieces) // GROUP
    steps = count_x // row_block
    channels = 3 * columns

    def kernel(*refs):
        info_ref, where_ref = refs[:2]
        piece_refs = refs[2 : 2 + pieces_n]
        out_ref = refs[2 + pieces_n]
        compact, total, staged, sems = refs[3 + pieces_n :]
        first_x = (lax.axis_index("rep") * lax.axis_size("pix") + lax.axis_index("pix")) * count_x
        first_z = lax.axis_index("slab") * planes
        tiles_max = segments * GROUP // TILE
        counts_at = segments + steps * tiles_max
        count = info_ref[counts_at + steps]
        tiles = (count + TILE // GROUP - 1) >> shift_of(TILE // GROUP)

        first = 0
        for piece in piece_refs:
            items = batch * planes // GROUP
            for start in range(0, piece.shape[0] // GROUP, items):
                targets = [info_ref[first + item] for item in range(items)]
                least = targets[0]
                for target in targets[1:]:
                    least = jnp.minimum(least, target)

                @pl.when(least < segments)
                def _(targets=targets, piece=piece, start=start):
                    for item, target in enumerate(targets):
                        rows = pl.ds(pl.multiple_of(target * GROUP, GROUP), GROUP)
                        source = (start + item) * GROUP
                        compact[rows, :] = piece[source : source + GROUP, :]

                first += items

        def clear(item, carry):
            target = pl.ds(pl.multiple_of(item * GROUP, GROUP), GROUP)
            compact[target, :] = jnp.zeros((GROUP, channels), jnp.bfloat16)
            return carry

        lax.fori_loop(count, tiles * (TILE // GROUP), clear, 0)

        def out_copy(step, slot):
            rows = pl.ds(step * row_block, row_block)
            return pltpu.make_async_copy(staged.at[slot], out_ref.at[rows], sems.at[slot])

        shape = (row_block, planes, columns)

        def one_step(step, carry):
            slot = step & 1

            def product(tile):
                lanes = pl.ds(pl.multiple_of(tile * TILE, TILE), TILE)
                lower_x, part_x = where_ref[0:1, lanes], where_ref[1:2, lanes]
                lower_z, part_z = where_ref[2:3, lanes], where_ref[3:4, lanes]
                at_x = first_x + step * row_block + lax.broadcasted_iota(jnp.int32, (row_block, TILE), 0)
                at_z = first_z + lax.broadcasted_iota(jnp.int32, (planes, TILE), 0)
                weight_x = corner(at_x.astype(jnp.float32), lower_x, part_x)
                weight_z = corner(at_z.astype(jnp.float32), lower_z, part_z)
                matrix = (weight_x[:, None, :] * weight_z[None, :, :]).astype(jnp.bfloat16)
                matrix = matrix.reshape(row_block * planes, TILE)
                return jnp.dot(matrix, compact[lanes, :], preferred_element_type=jnp.float32)

            touched = info_ref[counts_at + step]
            list_at = segments + step * tiles_max

            @pl.when(touched == 1)
            def _():
                total[...] = product(info_ref[list_at])

            @pl.when(touched >= 2)
            def _():
                total[...] = product(info_ref[list_at]) + product(info_ref[list_at + 1])

            def add(index, carry):
                total[...] += product(info_ref[list_at + index])
                return carry

            lax.fori_loop(2, touched, add, 0)

            @pl.when(step >= 2)
            def _():
                out_copy(step - 2, slot).wait()

            @pl.when(touched > 0)
            def _():
                scale = 1.0 / (total[:, 2 * columns :] + 1.0)
                staged[slot, :, :, :columns] = (total[:, :columns] * scale).reshape(shape)
                staged[slot, :, :, columns:] = (total[:, columns : 2 * columns] * scale).reshape(shape)

            @pl.when(touched == 0)
            def _():
                staged[slot] = jnp.zeros((row_block, planes, 2 * columns), jnp.float32)

            out_copy(step, slot).start()
            return carry

        lax.fori_loop(0, steps, one_step, 0)
        for step in range(max(steps - 2, 0), steps):
            out_copy(step, step % 2).wait()

    smem, vmem = pl.BlockSpec(memory_space=pltpu.SMEM), pl.BlockSpec(memory_space=pltpu.VMEM)
    return pl.pallas_call(
        kernel,
        out_shape=jax.ShapeDtypeStruct((count_x, planes, 2 * columns), jnp.float32),
        in_specs=[smem, vmem] + [vmem] * pieces_n,
        out_specs=pl.BlockSpec(memory_space=pl.ANY),
        scratch_shapes=[
            pltpu.VMEM((segments * GROUP + GROUP, channels), jnp.bfloat16),
            pltpu.VMEM((row_block * planes, channels), jnp.float32),
            pltpu.VMEM((2, row_block, planes, 2 * columns), jnp.float32),
            pltpu.SemaphoreType.DMA((2,)),
        ],
        compiler_params=pltpu.CompilerParams(vmem_limit_bytes=14 << 20),
        name="spread",
    )(info, where, *pieces)


def make_body(ports):
    def body(projections, ctf_weight, orient, angle_table):
        batch, planes = projections.shape[:2]
        columns = projections.shape[2] // 2
        count_x = columns // (ports.rep * ports.pix)
        row_block = TILE // planes
        sizes = (batch, planes, columns, count_x, row_block, ports.rep * ports.pix)
        samples = jnp.concatenate([projections, ctf_weight], axis=2).reshape(batch * planes, 3 * columns)
        pieces, owners, orients, orient_owners = gather_pieces(samples, orient, ports)
        info, where = make_plan(
            ports, orients, ports.distances(orient_owners), angle_table, ports.distances(owners), sizes
        )
        return spread(pieces, info, where, sizes)

    return body


def plain_body(projections, ctf_weight, orient, angle_table):
    planes = projections.shape[1]
    columns = projections.shape[2] // 2
    owned_rows = columns // (lax.axis_size("rep") * lax.axis_size("pix"))
    first_z = lax.axis_index("slab") * planes
    first_x = (lax.axis_index("rep") * lax.axis_size("pix") + lax.axis_index("pix")) * owned_rows
    samples = jnp.concatenate([projections, ctf_weight], axis=2)
    samples = lax.all_gather(samples, "slab", axis=1, tiled=True)
    samples = lax.all_gather(samples, BATCH_AXES, axis=0, tiled=True)
    geometry = lookup(lax.all_gather(orient, BATCH_AXES, axis=0, tiled=True), angle_table)
    geometry = geometry.astype(jnp.float32)
    at_x = (first_x + lax.iota(jnp.int32, owned_rows)).astype(jnp.float32)[:, None, None]
    at_z = (first_z + lax.iota(jnp.int32, planes)).astype(jnp.float32)[:, None, None]
    weight_x = corner(at_x, geometry[None, :, 0], geometry[None, :, 1] / 256.0)
    weight_z = corner(at_z, geometry[None, :, 2], geometry[None, :, 3] / 256.0)
    matrix = (weight_x[:, None] * weight_z[None]).astype(jnp.bfloat16).reshape(owned_rows * planes, -1)
    volume = jnp.dot(matrix, samples.reshape(-1, 3 * columns), preferred_element_type=jnp.float32)
    values = volume[:, : 2 * columns].reshape(-1, 2, columns) / (volume[:, None, 2 * columns :] + 1.0)
    return values.reshape(owned_rows, planes, 2 * columns)


def solution(mesh):
    placed = (
        P(BATCH_AXES, "slab", None),
        P(BATCH_AXES, "slab", None),
        P(BATCH_AXES),
        P(),
    )
    ports = Ports(mesh)

    def shard(body):
        return jax.shard_map(
            body, mesh=mesh, in_specs=placed, out_specs=P(BATCH_AXES, "slab", None), check_vma=False
        )

    if not ports.fits():
        return shard(plain_body)
    return shard(make_body(ports))
```

```python
import jax
import jax.numpy as jnp
import numpy as np
from jax import lax
from jax.experimental import pallas as pl
from jax.experimental.pallas import tpu as pltpu
from jax.sharding import PartitionSpec as P


BATCH_AXES = ("rep", "pix")
GROUP = 16
TILE = 256
LANES = 128


class Ports:
    def __init__(self, mesh):
        self.rep, self.slab, self.pix = (mesh.shape[a] for a in ("rep", "slab", "pix"))
        self.ids = np.arange(self.rep * self.slab * self.pix).reshape(self.rep, self.slab, self.pix)

    def fits(self):
        return (self.rep, self.slab, self.pix) == (2, 8, 2)

    def target(self, port, rep, slab, pix):
        if "|" in port:
            port = port.split("|")[pix]
        if port in ("x", "xy"):
            rep = 1 - rep
        if port in ("y", "xy"):
            slab = slab ^ 1
        if port == "z":
            slab = (slab + 2) % self.slab
        if port == "back":
            slab = (slab - 2) % self.slab
        if port == "core":
            pix = 1 - pix
        return self.ids[rep, slab, pix]

    def pairs(self, port):
        return [(int(self.ids[at]), int(self.target(port, *at))) for at in np.ndindex(self.ids.shape)]

    def move(self, owner, port):
        moved = np.empty_like(owner)
        for source, target in self.pairs(port):
            moved.flat[target] = owner.flat[source]
        return moved

    def send(self, held, port):
        value, owners = held
        value = lax.ppermute(value, ("rep", "slab", "pix"), self.pairs(port))
        return value, [self.move(owner, port) for owner in owners]

    def distances(self, owners):
        found = []
        for piece in range(owners.shape[-1]):
            per_core = []
            for pix in range(self.pix):
                rep, slab, core = np.unravel_index(owners[0, 0, pix, piece], self.ids.shape)
                per_core.append((int(rep), int(slab // 2), int(slab % 2), int(core) ^ pix))
            for at in np.ndindex(self.ids.shape):
                rep, slab, core = self.owner(per_core[at[2]], *at)
                assert self.ids[rep, slab, core] == owners[at][piece]
            found.append(per_core)
        return found

    def owner(self, distance, rep, slab, pix):
        far_x, far_z, far_y, far_core = distance
        upper = (slab // 2 + far_z) & (self.slab // 2 - 1)
        return rep ^ far_x, upper * 2 + ((slab & 1) ^ far_y), pix ^ far_core

    def both(self, held):
        other = self.send(held, "core")
        return other, (jnp.concatenate([held[0], other[0]], axis=0), held[1] + other[1])


def gather_pieces(samples, orient, ports):
    own = (samples, [ports.ids])
    core_own, chip_own = ports.both(own)
    up1 = ports.send(own, "z")
    side0 = ports.send(chip_own, "x|y")
    down = ports.send(own, "back")
    across = ports.send(own, "xy")
    orients = [(orient, [ports.ids])]
    orients.append(ports.send(orients[0], "core"))
    orients += [ports.send(orients[0], "x")]
    orients.append(ports.send(orients[2], "core"))
    core_up1, chip_up1 = ports.both(up1)
    up2 = ports.send(up1, "z")
    side1 = ports.send(chip_up1, "x|y")
    core_down, chip_down = ports.both(down)
    across1 = ports.send(across, "z")
    side3 = ports.send(chip_down, "x|y")
    across3 = ports.send(across, "back")
    core_up2, chip_up2 = ports.both(up2)
    side2 = ports.send(chip_up2, "x|y")
    across2 = ports.send(up2, "xy")
    pieces = [own, core_own, up1, core_up1, up2, core_up2, down, core_down]
    late = (across, side0, side1, across1, side3, across3, side2, across2)
    for held in late:
        pieces += [held, ports.send(held, "core")]
    owners = np.stack([owner for _, owned in pieces for owner in owned], axis=-1)
    assert (np.sort(owners, -1) == np.arange(ports.ids.size)).all()
    orient_owners = np.stack([owner for _, owned in orients for owner in owned], axis=-1)
    return [value for value, _ in pieces], owners, [value for value, _ in orients], orient_owners


def lookup(orient, angle_table):
    choose = (orient[:, None] == lax.iota(jnp.int32, angle_table.shape[0])[None, :]).astype(jnp.int32)
    return jnp.sum(choose[:, :, None, None] * angle_table[None], axis=1)


def corner(indices, lower, fraction):
    return jnp.where(indices == lower, 1.0 - fraction, 0.0) + jnp.where(indices == lower + 1, fraction, 0.0)


def shift_of(size):
    assert size & (size - 1) == 0
    return size.bit_length() - 1


def make_plan(ports, orients, orders, table, distances, sizes):
    batch, planes, columns, count_x, row_block, batches = sizes
    parts, pieces_n = len(orients), len(distances)
    items = batch * planes // GROUP
    segments = pieces_n * items
    steps, lane_groups = count_x // row_block, LANES // GROUP
    bits_at = 2 * segments
    tiles_max = segments * GROUP // TILE
    counts_at = segments + steps * tiles_max
    info_size = counts_at + steps + 1
    total_n = batch * batches

    def kernel(*refs):
        orient_refs = refs[:parts]
        table_ref, info_ref, where_ref, raw, geometry, found, found_s, listed, touched, sems = refs[parts:]
        rep, slab, pix = (lax.axis_index(axis) for axis in ("rep", "slab", "pix"))
        first_x = (rep * ports.pix + pix) * count_x
        first_z = slab * planes
        known = {}

        def place(per_core):
            for distance in per_core:
                if distance not in known:
                    at_rep, at_slab, at_pix = ports.owner(distance, rep, slab, pix)
                    known[distance] = (at_rep * ports.pix + at_pix) * batch, at_slab * (planes // GROUP)
            if len(set(per_core)) == 1:
                return known[per_core[0]]
            return [jnp.where(pix == 0, first, second) for first, second in zip(*(known[d] for d in per_core))]

        copies = [
            pltpu.make_async_copy(
                table_ref.at[orient_refs[n // batch][n % batch]], raw.at[n], sems.at[n]
            )
            for n in range(total_n)
        ]
        for copy in copies:
            copy.start()
        for copy in copies:
            copy.wait()
        unit = lax.broadcasted_iota(jnp.int32, (1, 4, columns), 1) & 1
        unit = jnp.where(unit[0] == 1, 1.0 / 256.0, 1.0)
        for n in range(total_n):
            geometry[place(orders[n // batch])[0] + n % batch, 0:4, :] = raw[n].astype(jnp.float32) * unit
        near_x = geometry[:, 0, :] - first_x.astype(jnp.float32)
        near_z = geometry[:, 2, :] - first_z.astype(jnp.float32)
        hit_z = (near_z >= -1.0) & (near_z < planes)
        hits = [
            jnp.where(hit_z & (near_x >= s * row_block - 1.0) & (near_x < (s + 1) * row_block), 1.0, 0.0)
            for s in range(steps)
        ]
        hits = jnp.concatenate(hits, axis=0).astype(jnp.bfloat16)
        lane = lax.broadcasted_iota(jnp.int32, (columns, LANES), 0)
        group = lax.broadcasted_iota(jnp.int32, (columns, LANES), 1)
        member = (lane // GROUP == group).astype(jnp.bfloat16)
        counted = jnp.dot(hits, member, preferred_element_type=jnp.float32)
        bits = jnp.zeros((total_n, LANES), jnp.float32)
        for s in range(steps):
            bits += jnp.where(counted[s * total_n : (s + 1) * total_n] > 0.0, float(2**s), 0.0)
        any_hit = jnp.where(bits > 0.0, 1.0, 0.0).astype(jnp.bfloat16)
        row = lax.broadcasted_iota(jnp.int32, (total_n, total_n), 0)
        col = lax.broadcasted_iota(jnp.int32, (total_n, total_n), 1)
        above = jnp.dot((col < row).astype(jnp.bfloat16), any_hit, preferred_element_type=jnp.float32)
        whole = jnp.dot(jnp.ones((total_n, total_n), jnp.bfloat16), any_hit, preferred_element_type=jnp.float32)
        row = lax.broadcasted_iota(jnp.int32, (LANES, LANES), 0)
        col = lax.broadcasted_iota(jnp.int32, (LANES, LANES), 1)
        before = jnp.dot(
            whole.astype(jnp.bfloat16), (row < col).astype(jnp.bfloat16), preferred_element_type=jnp.float32
        )
        code = jnp.where(bits > 0.0, bits * bits_at + above + before, 0.0)
        found[...] = code.astype(jnp.int32)
        to_scalar = pltpu.make_async_copy(found, found_s, sems.at[0])
        to_scalar.start()
        to_scalar.wait()

        for tile in range(tiles_max):
            touched[tile] = 0

        count = jnp.int32(0)
        for piece in range(pieces_n):
            first_n, first_g = place(distances[piece])
            for item in range(items):
                n, g = first_n + item // (items // batch), first_g + item % (items // batch)
                code = found_s[n, g]
                hit = code > 0
                listed[jnp.where(hit, code & (bits_at - 1), segments)] = n * LANES + g
                info_ref[piece * items + item] = jnp.where(hit, code & (bits_at - 1), segments)
                count += hit.astype(jnp.int32)
        info_ref[info_size - 1] = count
        tiles = (count + TILE // GROUP - 1) >> shift_of(TILE // GROUP)
        lane_group = lax.broadcasted_iota(jnp.int32, (8, LANES), 1) >> shift_of(GROUP)

        def order(block, carry):
            gathered = jnp.full((8, LANES), -4.0, jnp.float32)
            tile_bits = jnp.int32(0)
            for slot in range(lane_groups):
                index = block * lane_groups + slot
                valid = index < count
                name = listed[jnp.minimum(index, count - 1)]
                n, g = name >> shift_of(LANES), name & (LANES - 1)
                tile_bits |= found_s[n, g] >> shift_of(bits_at)
                lanes = pl.ds(pl.multiple_of((g >> shift_of(lane_groups)) * LANES, LANES), LANES)
                shift = ((slot - g) & (lane_groups - 1)) * GROUP
                rolled = pltpu.roll(geometry[n, :, lanes], shift, 1)
                gathered = jnp.where((lane_group == slot) & valid, rolled, gathered)
            where_ref[:, pl.ds(pl.multiple_of(block * LANES, LANES), LANES)] = gathered
            tile = block >> shift_of(TILE // LANES)
            touched[tile] = touched[tile] | tile_bits
            return carry

        lax.fori_loop(0, tiles * (TILE // LANES), order, 0)

        def to_steps(tile, counts):
            tile_bits = touched[tile]
            for s in range(steps):
                info_ref[segments + s * tiles_max + counts[s]] = tile
            return tuple(counts[s] + ((tile_bits >> s) & 1) for s in range(steps))

        counts = lax.fori_loop(0, tiles, to_steps, (jnp.int32(0),) * steps)
        for s in range(steps):
            info_ref[counts_at + s] = counts[s]

    smem, vmem = pl.BlockSpec(memory_space=pltpu.SMEM), pl.BlockSpec(memory_space=pltpu.VMEM)
    return pl.pallas_call(
        kernel,
        out_shape=[
            jax.ShapeDtypeStruct((info_size,), jnp.int32),
            jax.ShapeDtypeStruct((8, segments * GROUP), jnp.float32),
        ],
        in_specs=[smem] * parts + [pl.BlockSpec(memory_space=pl.ANY)],
        out_specs=[smem, vmem],
        scratch_shapes=[
            pltpu.VMEM((total_n, 4, columns), jnp.int32),
            pltpu.VMEM((total_n, 8, columns), jnp.float32),
            pltpu.VMEM((total_n, LANES), jnp.int32),
            pltpu.SMEM((total_n, LANES), jnp.int32),
            pltpu.SMEM((segments + 1,), jnp.int32),
            pltpu.SMEM((tiles_max,), jnp.int32),
            pltpu.SemaphoreType.DMA((total_n,)),
        ],
        compiler_params=pltpu.CompilerParams(vmem_limit_bytes=4 << 20),
        name="plan",
    )(*orients, table)


def spread(pieces, info, where, sizes):
    batch, planes, columns, count_x, row_block, _ = sizes
    pieces_n = len(pieces)
    segments = sum(piece.shape[0] for piece in pieces) // GROUP
    steps = count_x // row_block
    channels = 3 * columns

    def kernel(*refs):
        info_ref, where_ref = refs[:2]
        piece_refs = refs[2 : 2 + pieces_n]
        out_ref = refs[2 + pieces_n]
        compact, total, staged, sems = refs[3 + pieces_n :]
        first_x = (lax.axis_index("rep") * lax.axis_size("pix") + lax.axis_index("pix")) * count_x
        first_z = lax.axis_index("slab") * planes
        tiles_max = segments * GROUP // TILE
        counts_at = segments + steps * tiles_max
        count = info_ref[counts_at + steps]
        tiles = (count + TILE // GROUP - 1) >> shift_of(TILE // GROUP)

        first = 0
        for piece in piece_refs:
            items = batch * planes // GROUP
            for start in range(0, piece.shape[0] // GROUP, items):
                targets = [info_ref[first + item] for item in range(items)]
                least = targets[0]
                for target in targets[1:]:
                    least = jnp.minimum(least, target)

                @pl.when(least < segments)
                def _(targets=targets, piece=piece, start=start):
                    for item, target in enumerate(targets):
                        rows = pl.ds(pl.multiple_of(target * GROUP, GROUP), GROUP)
                        source = (start + item) * GROUP
                        compact[rows, :] = piece[source : source + GROUP, :]

                first += items

        def clear(item, carry):
            target = pl.ds(pl.multiple_of(item * GROUP, GROUP), GROUP)
            compact[target, :] = jnp.zeros((GROUP, channels), jnp.bfloat16)
            return carry

        lax.fori_loop(count, tiles * (TILE // GROUP), clear, 0)

        def out_copy(step, slot):
            rows = pl.ds(step * row_block, row_block)
            return pltpu.make_async_copy(staged.at[slot], out_ref.at[rows], sems.at[slot])

        shape = (row_block, planes, columns)

        def one_step(step, carry):
            slot = step & 3

            def product(tile):
                lanes = pl.ds(pl.multiple_of(tile * TILE, TILE), TILE)
                lower_x, part_x = where_ref[0:1, lanes], where_ref[1:2, lanes]
                lower_z, part_z = where_ref[2:3, lanes], where_ref[3:4, lanes]
                at_x = first_x + step * row_block + lax.broadcasted_iota(jnp.int32, (row_block, TILE), 0)
                at_z = first_z + lax.broadcasted_iota(jnp.int32, (planes, TILE), 0)
                weight_x = corner(at_x.astype(jnp.float32), lower_x, part_x)
                weight_z = corner(at_z.astype(jnp.float32), lower_z, part_z)
                matrix = (weight_x[:, None, :] * weight_z[None, :, :]).astype(jnp.bfloat16)
                matrix = matrix.reshape(row_block * planes, TILE)
                return jnp.dot(matrix, compact[lanes, :], preferred_element_type=jnp.float32)

            touched = info_ref[counts_at + step]
            list_at = segments + step * tiles_max

            @pl.when(touched == 1)
            def _():
                total[...] = product(info_ref[list_at])

            @pl.when(touched >= 2)
            def _():
                total[...] = product(info_ref[list_at]) + product(info_ref[list_at + 1])

            def add(index, carry):
                total[...] += product(info_ref[list_at + index])
                return carry

            lax.fori_loop(2, touched, add, 0)

            @pl.when(step >= 4)
            def _():
                out_copy(step - 4, slot).wait()

            @pl.when(touched > 0)
            def _():
                scale = 1.0 / (total[:, 2 * columns :] + 1.0)
                staged[slot, :, :, :columns] = (total[:, :columns] * scale).reshape(shape)
                staged[slot, :, :, columns:] = (total[:, columns : 2 * columns] * scale).reshape(shape)

            @pl.when(touched == 0)
            def _():
                staged[slot] = jnp.zeros((row_block, planes, 2 * columns), jnp.float32)

            out_copy(step, slot).start()
            return carry

        lax.fori_loop(0, steps, one_step, 0)
        for step in range(max(steps - 4, 0), steps):
            out_copy(step, step % 4).wait()

    smem, vmem = pl.BlockSpec(memory_space=pltpu.SMEM), pl.BlockSpec(memory_space=pltpu.VMEM)
    return pl.pallas_call(
        kernel,
        out_shape=jax.ShapeDtypeStruct((count_x, planes, 2 * columns), jnp.float32),
        in_specs=[smem, vmem] + [vmem] * pieces_n,
        out_specs=pl.BlockSpec(memory_space=pl.ANY),
        scratch_shapes=[
            pltpu.VMEM((segments * GROUP + GROUP, channels), jnp.bfloat16),
            pltpu.VMEM((row_block * planes, channels), jnp.float32),
            pltpu.VMEM((4, row_block, planes, 2 * columns), jnp.float32),
            pltpu.SemaphoreType.DMA((4,)),
        ],
        compiler_params=pltpu.CompilerParams(vmem_limit_bytes=14 << 20),
        name="spread",
    )(info, where, *pieces)


def make_body(ports):
    def body(projections, ctf_weight, orient, angle_table):
        batch, planes = projections.shape[:2]
        columns = projections.shape[2] // 2
        count_x = columns // (ports.rep * ports.pix)
        row_block = TILE // planes
        sizes = (batch, planes, columns, count_x, row_block, ports.rep * ports.pix)
        samples = jnp.concatenate([projections, ctf_weight], axis=2).reshape(batch * planes, 3 * columns)
        pieces, owners, orients, orient_owners = gather_pieces(samples, orient, ports)
        info, where = make_plan(
            ports, orients, ports.distances(orient_owners), angle_table, ports.distances(owners), sizes
        )
        return spread(pieces, info, where, sizes)

    return body


def plain_body(projections, ctf_weight, orient, angle_table):
    planes = projections.shape[1]
    columns = projections.shape[2] // 2
    owned_rows = columns // (lax.axis_size("rep") * lax.axis_size("pix"))
    first_z = lax.axis_index("slab") * planes
    first_x = (lax.axis_index("rep") * lax.axis_size("pix") + lax.axis_index("pix")) * owned_rows
    samples = jnp.concatenate([projections, ctf_weight], axis=2)
    samples = lax.all_gather(samples, "slab", axis=1, tiled=True)
    samples = lax.all_gather(samples, BATCH_AXES, axis=0, tiled=True)
    geometry = lookup(lax.all_gather(orient, BATCH_AXES, axis=0, tiled=True), angle_table)
    geometry = geometry.astype(jnp.float32)
    at_x = (first_x + lax.iota(jnp.int32, owned_rows)).astype(jnp.float32)[:, None, None]
    at_z = (first_z + lax.iota(jnp.int32, planes)).astype(jnp.float32)[:, None, None]
    weight_x = corner(at_x, geometry[None, :, 0], geometry[None, :, 1] / 256.0)
    weight_z = corner(at_z, geometry[None, :, 2], geometry[None, :, 3] / 256.0)
    matrix = (weight_x[:, None] * weight_z[None]).astype(jnp.bfloat16).reshape(owned_rows * planes, -1)
    volume = jnp.dot(matrix, samples.reshape(-1, 3 * columns), preferred_element_type=jnp.float32)
    values = volume[:, : 2 * columns].reshape(-1, 2, columns) / (volume[:, None, 2 * columns :] + 1.0)
    return values.reshape(owned_rows, planes, 2 * columns)


def solution(mesh):
    placed = (
        P(BATCH_AXES, "slab", None),
        P(BATCH_AXES, "slab", None),
        P(BATCH_AXES),
        P(),
    )
    ports = Ports(mesh)

    def shard(body):
        return jax.shard_map(
            body, mesh=mesh, in_specs=placed, out_specs=P(BATCH_AXES, "slab", None), check_vma=False
        )

    if not ports.fits():
        return shard(plain_body)
    return shard(make_body(ports))
```

```python
import jax
import jax.numpy as jnp
import numpy as np
from jax import lax
from jax.experimental import pallas as pl
from jax.experimental.pallas import tpu as pltpu
from jax.sharding import PartitionSpec as P


BATCH_AXES = ("rep", "pix")
GROUP = 16
TILE = 256
LANES = 128


class Ports:
    def __init__(self, mesh):
        self.rep, self.slab, self.pix = (mesh.shape[a] for a in ("rep", "slab", "pix"))
        self.ids = np.arange(self.rep * self.slab * self.pix).reshape(self.rep, self.slab, self.pix)

    def fits(self):
        return (self.rep, self.slab, self.pix) == (2, 8, 2)

    def target(self, port, rep, slab, pix):
        if "|" in port:
            port = port.split("|")[pix]
        if port in ("x", "xy"):
            rep = 1 - rep
        if port in ("y", "xy"):
            slab = slab ^ 1
        if port == "z":
            slab = (slab + 2) % self.slab
        if port == "back":
            slab = (slab - 2) % self.slab
        if port == "core":
            pix = 1 - pix
        return self.ids[rep, slab, pix]

    def pairs(self, port):
        return [(int(self.ids[at]), int(self.target(port, *at))) for at in np.ndindex(self.ids.shape)]

    def move(self, owner, port):
        moved = np.empty_like(owner)
        for source, target in self.pairs(port):
            moved.flat[target] = owner.flat[source]
        return moved

    def send(self, held, port):
        value, owners = held
        value = lax.ppermute(value, ("rep", "slab", "pix"), self.pairs(port))
        return value, [self.move(owner, port) for owner in owners]

    def distances(self, owners):
        found = []
        for piece in range(owners.shape[-1]):
            per_core = []
            for pix in range(self.pix):
                rep, slab, core = np.unravel_index(owners[0, 0, pix, piece], self.ids.shape)
                per_core.append((int(rep), int(slab // 2), int(slab % 2), int(core) ^ pix))
            for at in np.ndindex(self.ids.shape):
                rep, slab, core = self.owner(per_core[at[2]], *at)
                assert self.ids[rep, slab, core] == owners[at][piece]
            found.append(per_core)
        return found

    def owner(self, distance, rep, slab, pix):
        far_x, far_z, far_y, far_core = distance
        upper = (slab // 2 + far_z) & (self.slab // 2 - 1)
        return rep ^ far_x, upper * 2 + ((slab & 1) ^ far_y), pix ^ far_core

    def both(self, held):
        other = self.send(held, "core")
        return other, (jnp.concatenate([held[0], other[0]], axis=0), held[1] + other[1])


def gather_pieces(samples, orient, ports):
    own = (samples, [ports.ids])
    core_own, chip_own = ports.both(own)
    up1 = ports.send(own, "z")
    side0 = ports.send(chip_own, "x|y")
    down = ports.send(own, "back")
    across = ports.send(own, "xy")
    orients = [(orient, [ports.ids])]
    orients.append(ports.send(orients[0], "core"))
    orients += [ports.send(orients[0], "x")]
    orients.append(ports.send(orients[2], "core"))
    core_up1, chip_up1 = ports.both(up1)
    up2 = ports.send(up1, "z")
    side1 = ports.send(chip_up1, "x|y")
    core_down, chip_down = ports.both(down)
    across1 = ports.send(across, "z")
    side3 = ports.send(chip_down, "x|y")
    across3 = ports.send(across, "back")
    core_up2, chip_up2 = ports.both(up2)
    side2 = ports.send(chip_up2, "x|y")
    across2 = ports.send(up2, "xy")
    pieces = [own, core_own, up1, core_up1, up2, core_up2, down, core_down]
    late = (across, side0, side1, across1, side3, across3, across2, side2)
    for held in late:
        pieces += [held, ports.send(held, "core")]
    owners = np.stack([owner for _, owned in pieces for owner in owned], axis=-1)
    assert (np.sort(owners, -1) == np.arange(ports.ids.size)).all()
    orient_owners = np.stack([owner for _, owned in orients for owner in owned], axis=-1)
    return [value for value, _ in pieces], owners, [value for value, _ in orients], orient_owners


def lookup(orient, angle_table):
    choose = (orient[:, None] == lax.iota(jnp.int32, angle_table.shape[0])[None, :]).astype(jnp.int32)
    return jnp.sum(choose[:, :, None, None] * angle_table[None], axis=1)


def corner(indices, lower, fraction):
    return jnp.where(indices == lower, 1.0 - fraction, 0.0) + jnp.where(indices == lower + 1, fraction, 0.0)


def shift_of(size):
    assert size & (size - 1) == 0
    return size.bit_length() - 1


def make_plan(ports, orients, orders, table, distances, sizes):
    batch, planes, columns, count_x, row_block, batches = sizes
    parts, pieces_n = len(orients), len(distances)
    items = batch * planes // GROUP
    segments = pieces_n * items
    steps, lane_groups = count_x // row_block, LANES // GROUP
    bits_at = 2 * segments
    tiles_max = segments * GROUP // TILE
    counts_at = segments + steps * tiles_max
    info_size = counts_at + steps + 1
    total_n = batch * batches

    def kernel(*refs):
        orient_refs = refs[:parts]
        table_ref, info_ref, where_ref, raw, geometry, found, found_s, listed, touched, sems = refs[parts:]
        rep, slab, pix = (lax.axis_index(axis) for axis in ("rep", "slab", "pix"))
        first_x = (rep * ports.pix + pix) * count_x
        first_z = slab * planes
        known = {}

        def place(per_core):
            for distance in per_core:
                if distance not in known:
                    at_rep, at_slab, at_pix = ports.owner(distance, rep, slab, pix)
                    known[distance] = (at_rep * ports.pix + at_pix) * batch, at_slab * (planes // GROUP)
            if len(set(per_core)) == 1:
                return known[per_core[0]]
            return [jnp.where(pix == 0, first, second) for first, second in zip(*(known[d] for d in per_core))]

        copies = [
            pltpu.make_async_copy(
                table_ref.at[orient_refs[n // batch][n % batch]], raw.at[n], sems.at[n]
            )
            for n in range(total_n)
        ]
        for copy in copies:
            copy.start()
        for copy in copies:
            copy.wait()
        unit = lax.broadcasted_iota(jnp.int32, (1, 4, columns), 1) & 1
        unit = jnp.where(unit[0] == 1, 1.0 / 256.0, 1.0)
        for n in range(total_n):
            geometry[place(orders[n // batch])[0] + n % batch, 0:4, :] = raw[n].astype(jnp.float32) * unit
        near_x = geometry[:, 0, :] - first_x.astype(jnp.float32)
        near_z = geometry[:, 2, :] - first_z.astype(jnp.float32)
        hit_z = (near_z >= -1.0) & (near_z < planes)
        hits = [
            jnp.where(hit_z & (near_x >= s * row_block - 1.0) & (near_x < (s + 1) * row_block), 1.0, 0.0)
            for s in range(steps)
        ]
        hits = jnp.concatenate(hits, axis=0).astype(jnp.bfloat16)
        lane = lax.broadcasted_iota(jnp.int32, (columns, LANES), 0)
        group = lax.broadcasted_iota(jnp.int32, (columns, LANES), 1)
        member = (lane // GROUP == group).astype(jnp.bfloat16)
        counted = jnp.dot(hits, member, preferred_element_type=jnp.float32)
        bits = jnp.zeros((total_n, LANES), jnp.float32)
        for s in range(steps):
            bits += jnp.where(counted[s * total_n : (s + 1) * total_n] > 0.0, float(2**s), 0.0)
        any_hit = jnp.where(bits > 0.0, 1.0, 0.0).astype(jnp.bfloat16)
        row = lax.broadcasted_iota(jnp.int32, (total_n, total_n), 0)
        col = lax.broadcasted_iota(jnp.int32, (total_n, total_n), 1)
        above = jnp.dot((col < row).astype(jnp.bfloat16), any_hit, preferred_element_type=jnp.float32)
        whole = jnp.dot(jnp.ones((total_n, total_n), jnp.bfloat16), any_hit, preferred_element_type=jnp.float32)
        row = lax.broadcasted_iota(jnp.int32, (LANES, LANES), 0)
        col = lax.broadcasted_iota(jnp.int32, (LANES, LANES), 1)
        before = jnp.dot(
            whole.astype(jnp.bfloat16), (row < col).astype(jnp.bfloat16), preferred_element_type=jnp.float32
        )
        code = jnp.where(bits > 0.0, bits * bits_at + above + before, 0.0)
        found[...] = code.astype(jnp.int32)
        to_scalar = pltpu.make_async_copy(found, found_s, sems.at[0])
        to_scalar.start()
        to_scalar.wait()

        for tile in range(tiles_max):
            touched[tile] = 0

        count = jnp.int32(0)
        for piece in range(pieces_n):
            first_n, first_g = place(distances[piece])
            for item in range(items):
                n, g = first_n + item // (items // batch), first_g + item % (items // batch)
                code = found_s[n, g]
                hit = code > 0
                listed[jnp.where(hit, code & (bits_at - 1), segments)] = n * LANES + g
                info_ref[piece * items + item] = jnp.where(hit, code & (bits_at - 1), segments)
                count += hit.astype(jnp.int32)
        info_ref[info_size - 1] = count
        tiles = (count + TILE // GROUP - 1) >> shift_of(TILE // GROUP)
        lane_group = lax.broadcasted_iota(jnp.int32, (8, LANES), 1) >> shift_of(GROUP)

        def order(block, carry):
            gathered = jnp.full((8, LANES), -4.0, jnp.float32)
            tile_bits = jnp.int32(0)
            for slot in range(lane_groups):
                index = block * lane_groups + slot
                valid = index < count
                name = listed[jnp.minimum(index, count - 1)]
                n, g = name >> shift_of(LANES), name & (LANES - 1)
                tile_bits |= found_s[n, g] >> shift_of(bits_at)
                lanes = pl.ds(pl.multiple_of((g >> shift_of(lane_groups)) * LANES, LANES), LANES)
                shift = ((slot - g) & (lane_groups - 1)) * GROUP
                rolled = pltpu.roll(geometry[n, :, lanes], shift, 1)
                gathered = jnp.where((lane_group == slot) & valid, rolled, gathered)
            where_ref[:, pl.ds(pl.multiple_of(block * LANES, LANES), LANES)] = gathered
            tile = block >> shift_of(TILE // LANES)
            touched[tile] = touched[tile] | tile_bits
            return carry

        lax.fori_loop(0, tiles * (TILE // LANES), order, 0)

        def to_steps(tile, counts):
            tile_bits = touched[tile]
            for s in range(steps):
                info_ref[segments + s * tiles_max + counts[s]] = tile
            return tuple(counts[s] + ((tile_bits >> s) & 1) for s in range(steps))

        counts = lax.fori_loop(0, tiles, to_steps, (jnp.int32(0),) * steps)
        for s in range(steps):
            info_ref[counts_at + s] = counts[s]

    smem, vmem = pl.BlockSpec(memory_space=pltpu.SMEM), pl.BlockSpec(memory_space=pltpu.VMEM)
    return pl.pallas_call(
        kernel,
        out_shape=[
            jax.ShapeDtypeStruct((info_size,), jnp.int32),
            jax.ShapeDtypeStruct((8, segments * GROUP), jnp.float32),
        ],
        in_specs=[smem] * parts + [pl.BlockSpec(memory_space=pl.ANY)],
        out_specs=[smem, vmem],
        scratch_shapes=[
            pltpu.VMEM((total_n, 4, columns), jnp.int32),
            pltpu.VMEM((total_n, 8, columns), jnp.float32),
            pltpu.VMEM((total_n, LANES), jnp.int32),
            pltpu.SMEM((total_n, LANES), jnp.int32),
            pltpu.SMEM((segments + 1,), jnp.int32),
            pltpu.SMEM((tiles_max,), jnp.int32),
            pltpu.SemaphoreType.DMA((total_n,)),
        ],
        compiler_params=pltpu.CompilerParams(vmem_limit_bytes=4 << 20),
        name="plan",
    )(*orients, table)


def copy_groups(info_ref, compact, piece_refs, first, segments, items):
    for piece in piece_refs:
        for start in range(0, piece.shape[0] // GROUP, items):
            targets = [info_ref[first + item] for item in range(items)]
            least = targets[0]
            for target in targets[1:]:
                least = jnp.minimum(least, target)

            @pl.when(least < segments)
            def _(targets=targets, piece=piece, start=start):
                for item, target in enumerate(targets):
                    rows = pl.ds(pl.multiple_of(target * GROUP, GROUP), GROUP)
                    source = (start + item) * GROUP
                    compact[rows, :] = piece[source : source + GROUP, :]

            first += items


def collect(pieces, info, segments, sizes):
    batch, planes, columns = sizes[:3]
    channels = 3 * columns

    def kernel(*refs):
        info_ref, piece_refs, compact = refs[0], refs[1:-1], refs[-1]
        count = info_ref[info.shape[0] - 1]
        tiles = (count + TILE // GROUP - 1) >> shift_of(TILE // GROUP)

        def clear(item, carry):
            target = pl.ds(pl.multiple_of(item * GROUP, GROUP), GROUP)
            compact[target, :] = jnp.zeros((GROUP, channels), jnp.bfloat16)
            return carry

        lax.fori_loop(count, tiles * (TILE // GROUP), clear, 0)
        copy_groups(info_ref, compact, piece_refs, 0, segments, batch * planes // GROUP)

    smem, vmem = pl.BlockSpec(memory_space=pltpu.SMEM), pl.BlockSpec(memory_space=pltpu.VMEM)
    return pl.pallas_call(
        kernel,
        out_shape=jax.ShapeDtypeStruct((segments * GROUP + GROUP, channels), jnp.bfloat16),
        in_specs=[smem] + [vmem] * len(pieces),
        out_specs=vmem,
        compiler_params=pltpu.CompilerParams(vmem_limit_bytes=8 << 20),
        name="collect",
    )(info, *pieces)


def spread(compact, pieces, info, where, segments, sizes):
    batch, planes, columns, count_x, row_block, _ = sizes
    pieces_n = len(pieces)
    first_segment = segments - sum(piece.shape[0] for piece in pieces) // GROUP
    steps = count_x // row_block
    channels = 3 * columns

    def kernel(*refs):
        info_ref, where_ref = refs[:2]
        piece_refs = refs[3 : 3 + pieces_n]
        out_ref, compact, total, staged, sems = refs[3 + pieces_n :]
        first_x = (lax.axis_index("rep") * lax.axis_size("pix") + lax.axis_index("pix")) * count_x
        first_z = lax.axis_index("slab") * planes
        tiles_max = segments * GROUP // TILE
        counts_at = segments + steps * tiles_max
        copy_groups(info_ref, compact, piece_refs, first_segment, segments, batch * planes // GROUP)

        def out_copy(step, slot):
            rows = pl.ds(step * row_block, row_block)
            return pltpu.make_async_copy(staged.at[slot], out_ref.at[rows], sems.at[slot])

        shape = (row_block, planes, columns)

        def one_step(step, carry):
            slot = step & 3

            def product(tile):
                lanes = pl.ds(pl.multiple_of(tile * TILE, TILE), TILE)
                lower_x, part_x = where_ref[0:1, lanes], where_ref[1:2, lanes]
                lower_z, part_z = where_ref[2:3, lanes], where_ref[3:4, lanes]
                at_x = first_x + step * row_block + lax.broadcasted_iota(jnp.int32, (row_block, TILE), 0)
                at_z = first_z + lax.broadcasted_iota(jnp.int32, (planes, TILE), 0)
                weight_x = corner(at_x.astype(jnp.float32), lower_x, part_x)
                weight_z = corner(at_z.astype(jnp.float32), lower_z, part_z)
                matrix = (weight_x[:, None, :] * weight_z[None, :, :]).astype(jnp.bfloat16)
                matrix = matrix.reshape(row_block * planes, TILE)
                return jnp.dot(matrix, compact[lanes, :], preferred_element_type=jnp.float32)

            touched = info_ref[counts_at + step]
            list_at = segments + step * tiles_max

            @pl.when(touched == 1)
            def _():
                total[...] = product(info_ref[list_at])

            @pl.when(touched >= 2)
            def _():
                total[...] = product(info_ref[list_at]) + product(info_ref[list_at + 1])

            def add(index, carry):
                total[...] += product(info_ref[list_at + index])
                return carry

            lax.fori_loop(2, touched, add, 0)

            @pl.when(step >= 4)
            def _():
                out_copy(step - 4, slot).wait()

            @pl.when(touched > 0)
            def _():
                scale = 1.0 / (total[:, 2 * columns :] + 1.0)
                staged[slot, :, :, :columns] = (total[:, :columns] * scale).reshape(shape)
                staged[slot, :, :, columns:] = (total[:, columns : 2 * columns] * scale).reshape(shape)

            @pl.when(touched == 0)
            def _():
                staged[slot] = jnp.zeros((row_block, planes, 2 * columns), jnp.float32)

            out_copy(step, slot).start()
            return carry

        lax.fori_loop(0, steps, one_step, 0)
        for step in range(max(steps - 4, 0), steps):
            out_copy(step, step % 4).wait()

    smem, vmem = pl.BlockSpec(memory_space=pltpu.SMEM), pl.BlockSpec(memory_space=pltpu.VMEM)
    return pl.pallas_call(
        kernel,
        out_shape=[
            jax.ShapeDtypeStruct((count_x, planes, 2 * columns), jnp.float32),
            jax.ShapeDtypeStruct(compact.shape, compact.dtype),
        ],
        in_specs=[smem, vmem, vmem] + [vmem] * pieces_n,
        out_specs=[pl.BlockSpec(memory_space=pl.ANY), vmem],
        input_output_aliases={2: 1},
        scratch_shapes=[
            pltpu.VMEM((row_block * planes, channels), jnp.float32),
            pltpu.VMEM((4, row_block, planes, 2 * columns), jnp.float32),
            pltpu.SemaphoreType.DMA((4,)),
        ],
        compiler_params=pltpu.CompilerParams(vmem_limit_bytes=14 << 20),
        name="spread",
    )(info, where, compact, *pieces)[0]


def make_body(ports):
    def body(projections, ctf_weight, orient, angle_table):
        batch, planes = projections.shape[:2]
        columns = projections.shape[2] // 2
        count_x = columns // (ports.rep * ports.pix)
        row_block = TILE // planes
        sizes = (batch, planes, columns, count_x, row_block, ports.rep * ports.pix)
        samples = jnp.concatenate([projections, ctf_weight], axis=2).reshape(batch * planes, 3 * columns)
        pieces, owners, orients, orient_owners = gather_pieces(samples, orient, ports)
        info, where = make_plan(
            ports, orients, ports.distances(orient_owners), angle_table, ports.distances(owners), sizes
        )
        segments = owners.shape[-1] * (batch * planes // GROUP)
        compact = collect(pieces[:-1], info, segments, sizes)
        return spread(compact, pieces[-1:], info, where, segments, sizes)

    return body


def plain_body(projections, ctf_weight, orient, angle_table):
    planes = projections.shape[1]
    columns = projections.shape[2] // 2
    owned_rows = columns // (lax.axis_size("rep") * lax.axis_size("pix"))
    first_z = lax.axis_index("slab") * planes
    first_x = (lax.axis_index("rep") * lax.axis_size("pix") + lax.axis_index("pix")) * owned_rows
    samples = jnp.concatenate([projections, ctf_weight], axis=2)
    samples = lax.all_gather(samples, "slab", axis=1, tiled=True)
    samples = lax.all_gather(samples, BATCH_AXES, axis=0, tiled=True)
    geometry = lookup(lax.all_gather(orient, BATCH_AXES, axis=0, tiled=True), angle_table)
    geometry = geometry.astype(jnp.float32)
    at_x = (first_x + lax.iota(jnp.int32, owned_rows)).astype(jnp.float32)[:, None, None]
    at_z = (first_z + lax.iota(jnp.int32, planes)).astype(jnp.float32)[:, None, None]
    weight_x = corner(at_x, geometry[None, :, 0], geometry[None, :, 1] / 256.0)
    weight_z = corner(at_z, geometry[None, :, 2], geometry[None, :, 3] / 256.0)
    matrix = (weight_x[:, None] * weight_z[None]).astype(jnp.bfloat16).reshape(owned_rows * planes, -1)
    volume = jnp.dot(matrix, samples.reshape(-1, 3 * columns), preferred_element_type=jnp.float32)
    values = volume[:, : 2 * columns].reshape(-1, 2, columns) / (volume[:, None, 2 * columns :] + 1.0)
    return values.reshape(owned_rows, planes, 2 * columns)


def solution(mesh):
    placed = (
        P(BATCH_AXES, "slab", None),
        P(BATCH_AXES, "slab", None),
        P(BATCH_AXES),
        P(),
    )
    ports = Ports(mesh)

    def shard(body):
        return jax.shard_map(
            body, mesh=mesh, in_specs=placed, out_specs=P(BATCH_AXES, "slab", None), check_vma=False
        )

    if not ports.fits():
        return shard(plain_body)
    return shard(make_body(ports))
```

```python
import jax
import jax.numpy as jnp
import numpy as np
from jax import lax
from jax.experimental import pallas as pl
from jax.experimental.pallas import tpu as pltpu
from jax.sharding import PartitionSpec as P


BATCH_AXES = ("rep", "pix")
GROUP = 16
TILE = 256
LANES = 128


class Ports:
    def __init__(self, mesh):
        self.rep, self.slab, self.pix = (mesh.shape[a] for a in ("rep", "slab", "pix"))
        self.ids = np.arange(self.rep * self.slab * self.pix).reshape(self.rep, self.slab, self.pix)

    def fits(self):
        return (self.rep, self.slab, self.pix) == (2, 8, 2)

    def target(self, port, rep, slab, pix):
        if "|" in port:
            port = port.split("|")[pix]
        if port in ("x", "xy"):
            rep = 1 - rep
        if port in ("y", "xy"):
            slab = slab ^ 1
        if port == "z":
            slab = (slab + 2) % self.slab
        if port == "back":
            slab = (slab - 2) % self.slab
        if port == "core":
            pix = 1 - pix
        return self.ids[rep, slab, pix]

    def pairs(self, port):
        return [(int(self.ids[at]), int(self.target(port, *at))) for at in np.ndindex(self.ids.shape)]

    def move(self, owner, port):
        moved = np.empty_like(owner)
        for source, target in self.pairs(port):
            moved.flat[target] = owner.flat[source]
        return moved

    def send(self, held, port):
        value, owners = held
        value = lax.ppermute(value, ("rep", "slab", "pix"), self.pairs(port))
        return value, [self.move(owner, port) for owner in owners]

    def distances(self, owners):
        found = []
        for piece in range(owners.shape[-1]):
            per_core = []
            for pix in range(self.pix):
                rep, slab, core = np.unravel_index(owners[0, 0, pix, piece], self.ids.shape)
                per_core.append((int(rep), int(slab // 2), int(slab % 2), int(core) ^ pix))
            for at in np.ndindex(self.ids.shape):
                rep, slab, core = self.owner(per_core[at[2]], *at)
                assert self.ids[rep, slab, core] == owners[at][piece]
            found.append(per_core)
        return found

    def owner(self, distance, rep, slab, pix):
        far_x, far_z, far_y, far_core = distance
        upper = (slab // 2 + far_z) & (self.slab // 2 - 1)
        return rep ^ far_x, upper * 2 + ((slab & 1) ^ far_y), pix ^ far_core

    def both(self, held):
        other = self.send(held, "core")
        return other, (jnp.concatenate([held[0], other[0]], axis=0), held[1] + other[1])


def gather_pieces(samples, orient, ports):
    own = (samples, [ports.ids])
    core_own, chip_own = ports.both(own)
    up1 = ports.send(own, "z")
    side0 = ports.send(chip_own, "x|y")
    down = ports.send(own, "back")
    across = ports.send(own, "xy")
    orients = [(orient, [ports.ids])]
    orients.append(ports.send(orients[0], "core"))
    orients += [ports.send(orients[0], "x")]
    orients.append(ports.send(orients[2], "core"))
    orients[0] = ports.send(orients[1], "core")
    core_up1, chip_up1 = ports.both(up1)
    up2 = ports.send(up1, "z")
    side1 = ports.send(chip_up1, "x|y")
    core_down, chip_down = ports.both(down)
    across1 = ports.send(across, "z")
    side3 = ports.send(chip_down, "x|y")
    across3 = ports.send(across, "back")
    core_up2, chip_up2 = ports.both(up2)
    side2 = ports.send(chip_up2, "x|y")
    across2 = ports.send(up2, "xy")
    pieces = [own, core_own, up1, core_up1, up2, core_up2, down, core_down]
    late = (across, side0, side1, across1, side3, across3, across2, side2)
    for held in late:
        pieces += [held, ports.send(held, "core")]
    owners = np.stack([owner for _, owned in pieces for owner in owned], axis=-1)
    assert (np.sort(owners, -1) == np.arange(ports.ids.size)).all()
    orient_owners = np.stack([owner for _, owned in orients for owner in owned], axis=-1)
    return [value for value, _ in pieces], owners, [value for value, _ in orients], orient_owners


def lookup(orient, angle_table):
    choose = (orient[:, None] == lax.iota(jnp.int32, angle_table.shape[0])[None, :]).astype(jnp.int32)
    return jnp.sum(choose[:, :, None, None] * angle_table[None], axis=1)


def corner(indices, lower, fraction):
    return jnp.where(indices == lower, 1.0 - fraction, 0.0) + jnp.where(indices == lower + 1, fraction, 0.0)


def shift_of(size):
    assert size & (size - 1) == 0
    return size.bit_length() - 1


def make_plan(ports, orients, orders, table, distances, sizes):
    batch, planes, columns, count_x, row_block, batches = sizes
    parts, pieces_n = len(orients), len(distances)
    items = batch * planes // GROUP
    segments = pieces_n * items
    steps, lane_groups = count_x // row_block, LANES // GROUP
    bits_at = 2 * segments
    tiles_max = segments * GROUP // TILE
    counts_at = segments + steps * tiles_max
    info_size = counts_at + steps + 1
    total_n = batch * batches

    def kernel(*refs):
        orient_refs = refs[:parts]
        table_ref, info_ref, where_ref, out_ref = refs[parts : parts + 4]
        raw, geometry, found, found_s, listed, touched, zeros, sems, zero_sems = refs[parts + 4 :]

        rep, slab, pix = (lax.axis_index(axis) for axis in ("rep", "slab", "pix"))
        first_x = (rep * ports.pix + pix) * count_x
        first_z = slab * planes
        known = {}

        def place(per_core):
            for distance in per_core:
                if distance not in known:
                    at_rep, at_slab, at_pix = ports.owner(distance, rep, slab, pix)
                    known[distance] = (at_rep * ports.pix + at_pix) * batch, at_slab * (planes // GROUP)
            if len(set(per_core)) == 1:
                return known[per_core[0]]
            return [jnp.where(pix == 0, first, second) for first, second in zip(*(known[d] for d in per_core))]

        copies = [
            pltpu.make_async_copy(
                table_ref.at[orient_refs[n // batch][n % batch]], raw.at[n], sems.at[n]
            )
            for n in range(total_n)
        ]
        for copy in copies:
            copy.start()
        for copy in copies:
            copy.wait()
        unit = lax.broadcasted_iota(jnp.int32, (1, 4, columns), 1) & 1
        unit = jnp.where(unit[0] == 1, 1.0 / 256.0, 1.0)
        for n in range(total_n):
            geometry[place(orders[n // batch])[0] + n % batch, 0:4, :] = raw[n].astype(jnp.float32) * unit
        near_x = geometry[:, 0, :] - first_x.astype(jnp.float32)
        near_z = geometry[:, 2, :] - first_z.astype(jnp.float32)
        hit_z = (near_z >= -1.0) & (near_z < planes)
        hits = [
            jnp.where(hit_z & (near_x >= s * row_block - 1.0) & (near_x < (s + 1) * row_block), 1.0, 0.0)
            for s in range(steps)
        ]
        hits = jnp.concatenate(hits, axis=0).astype(jnp.bfloat16)
        lane = lax.broadcasted_iota(jnp.int32, (columns, LANES), 0)
        group = lax.broadcasted_iota(jnp.int32, (columns, LANES), 1)
        member = (lane // GROUP == group).astype(jnp.bfloat16)
        counted = jnp.dot(hits, member, preferred_element_type=jnp.float32)
        bits = jnp.zeros((total_n, LANES), jnp.float32)
        for s in range(steps):
            bits += jnp.where(counted[s * total_n : (s + 1) * total_n] > 0.0, float(2**s), 0.0)
        any_hit = jnp.where(bits > 0.0, 1.0, 0.0).astype(jnp.bfloat16)
        row = lax.broadcasted_iota(jnp.int32, (total_n, total_n), 0)
        col = lax.broadcasted_iota(jnp.int32, (total_n, total_n), 1)
        above = jnp.dot((col < row).astype(jnp.bfloat16), any_hit, preferred_element_type=jnp.float32)
        whole = jnp.dot(jnp.ones((total_n, total_n), jnp.bfloat16), any_hit, preferred_element_type=jnp.float32)
        row = lax.broadcasted_iota(jnp.int32, (LANES, LANES), 0)
        col = lax.broadcasted_iota(jnp.int32, (LANES, LANES), 1)
        before = jnp.dot(
            whole.astype(jnp.bfloat16), (row < col).astype(jnp.bfloat16), preferred_element_type=jnp.float32
        )
        code = jnp.where(bits > 0.0, bits * bits_at + above + before, 0.0)
        found[:total_n] = code.astype(jnp.int32)
        hit_groups = jnp.where(counted > 0.0, 1.0, 0.0).astype(jnp.bfloat16)
        row = lax.broadcasted_iota(jnp.int32, (8, steps * total_n), 0)
        col = lax.broadcasted_iota(jnp.int32, (8, steps * total_n), 1)
        of_step = (col >> shift_of(total_n) == row).astype(jnp.bfloat16)
        per_group = jnp.dot(of_step, hit_groups, preferred_element_type=jnp.float32).astype(jnp.bfloat16)
        per_step = jnp.dot(per_group, jnp.ones((LANES, LANES), jnp.bfloat16), preferred_element_type=jnp.float32)
        found[total_n:] = per_step.astype(jnp.int32)
        zeros[...] = jnp.zeros_like(zeros)
        to_scalar = pltpu.make_async_copy(found, found_s, sems.at[0])
        to_scalar.start()
        to_scalar.wait()

        def zero_copy(step):
            return pltpu.make_async_copy(zeros, out_ref.at[pl.ds(step * row_block, row_block)], zero_sems.at[step])

        for step in range(steps):

            @pl.when(found_s[total_n + step, 0] == 0)
            def _(step=step):
                zero_copy(step).start()

        for tile in range(tiles_max):
            touched[tile] = 0

        count = jnp.int32(0)
        for piece in range(pieces_n):
            first_n, first_g = place(distances[piece])
            for item in range(items):
                n, g = first_n + item // (items // batch), first_g + item % (items // batch)
                code = found_s[n, g]
                hit = code > 0
                listed[jnp.where(hit, code & (bits_at - 1), segments)] = n * LANES + g
                info_ref[piece * items + item] = jnp.where(hit, code & (bits_at - 1), segments)
                count += hit.astype(jnp.int32)
        info_ref[info_size - 1] = count
        tiles = (count + TILE // GROUP - 1) >> shift_of(TILE // GROUP)
        lane_group = lax.broadcasted_iota(jnp.int32, (8, LANES), 1) >> shift_of(GROUP)

        def order(block, carry):
            gathered = jnp.full((8, LANES), -4.0, jnp.float32)
            tile_bits = jnp.int32(0)
            for slot in range(lane_groups):
                index = block * lane_groups + slot
                valid = index < count
                name = listed[jnp.minimum(index, count - 1)]
                n, g = name >> shift_of(LANES), name & (LANES - 1)
                tile_bits |= found_s[n, g] >> shift_of(bits_at)
                lanes = pl.ds(pl.multiple_of((g >> shift_of(lane_groups)) * LANES, LANES), LANES)
                shift = ((slot - g) & (lane_groups - 1)) * GROUP
                rolled = pltpu.roll(geometry[n, :, lanes], shift, 1)
                gathered = jnp.where((lane_group == slot) & valid, rolled, gathered)
            where_ref[:, pl.ds(pl.multiple_of(block * LANES, LANES), LANES)] = gathered
            tile = block >> shift_of(TILE // LANES)
            touched[tile] = touched[tile] | tile_bits
            return carry

        lax.fori_loop(0, tiles * (TILE // LANES), order, 0)

        def to_steps(tile, counts):
            tile_bits = touched[tile]
            for s in range(steps):
                info_ref[segments + s * tiles_max + counts[s]] = tile
            return tuple(counts[s] + ((tile_bits >> s) & 1) for s in range(steps))

        counts = lax.fori_loop(0, tiles, to_steps, (jnp.int32(0),) * steps)
        for s in range(steps):
            info_ref[counts_at + s] = counts[s]
        for step in range(steps):

            @pl.when(found_s[total_n + step, 0] == 0)
            def _(step=step):
                zero_copy(step).wait()

    smem, vmem = pl.BlockSpec(memory_space=pltpu.SMEM), pl.BlockSpec(memory_space=pltpu.VMEM)
    return pl.pallas_call(
        kernel,
        out_shape=[
            jax.ShapeDtypeStruct((info_size,), jnp.int32),
            jax.ShapeDtypeStruct((8, segments * GROUP), jnp.float32),
            jax.ShapeDtypeStruct((count_x, planes, 2 * columns), jnp.float32),
        ],
        in_specs=[smem] * parts + [pl.BlockSpec(memory_space=pl.ANY)],
        out_specs=[smem, vmem, pl.BlockSpec(memory_space=pl.ANY)],
        scratch_shapes=[
            pltpu.VMEM((total_n, 4, columns), jnp.int32),
            pltpu.VMEM((total_n, 8, columns), jnp.float32),
            pltpu.VMEM((total_n + 8, LANES), jnp.int32),
            pltpu.SMEM((total_n + 8, LANES), jnp.int32),
            pltpu.SMEM((segments + 1,), jnp.int32),
            pltpu.SMEM((tiles_max,), jnp.int32),
            pltpu.VMEM((row_block, planes, 2 * columns), jnp.float32),
            pltpu.SemaphoreType.DMA((total_n,)),
            pltpu.SemaphoreType.DMA((steps,)),
        ],
        compiler_params=pltpu.CompilerParams(vmem_limit_bytes=4 << 20),
        name="plan",
    )(*orients, table)


def copy_groups(info_ref, compact, piece_refs, first, segments, items):
    for piece in piece_refs:
        for start in range(0, piece.shape[0] // GROUP, items):
            targets = [info_ref[first + item] for item in range(items)]
            least = targets[0]
            for target in targets[1:]:
                least = jnp.minimum(least, target)

            @pl.when(least < segments)
            def _(targets=targets, piece=piece, start=start):
                for item, target in enumerate(targets):
                    rows = pl.ds(pl.multiple_of(target * GROUP, GROUP), GROUP)
                    source = (start + item) * GROUP
                    compact[rows, :] = piece[source : source + GROUP, :]

            first += items


def collect(pieces, info, segments, sizes):
    batch, planes, columns = sizes[:3]
    channels = 3 * columns

    def kernel(*refs):
        info_ref, piece_refs, compact = refs[0], refs[1:-1], refs[-1]
        count = info_ref[info.shape[0] - 1]
        tiles = (count + TILE // GROUP - 1) >> shift_of(TILE // GROUP)

        def clear(item, carry):
            target = pl.ds(pl.multiple_of(item * GROUP, GROUP), GROUP)
            compact[target, :] = jnp.zeros((GROUP, channels), jnp.bfloat16)
            return carry

        lax.fori_loop(count, tiles * (TILE // GROUP), clear, 0)
        copy_groups(info_ref, compact, piece_refs, 0, segments, batch * planes // GROUP)

    smem, vmem = pl.BlockSpec(memory_space=pltpu.SMEM), pl.BlockSpec(memory_space=pltpu.VMEM)
    return pl.pallas_call(
        kernel,
        out_shape=jax.ShapeDtypeStruct((segments * GROUP + GROUP, channels), jnp.bfloat16),
        in_specs=[smem] + [vmem] * len(pieces),
        out_specs=vmem,
        compiler_params=pltpu.CompilerParams(vmem_limit_bytes=8 << 20),
        name="collect",
    )(info, *pieces)


def spread(compact, density, pieces, info, where, segments, sizes):
    batch, planes, columns, count_x, row_block, _ = sizes
    pieces_n = len(pieces)
    first_segment = segments - sum(piece.shape[0] for piece in pieces) // GROUP
    steps = count_x // row_block
    channels = 3 * columns

    def kernel(*refs):
        info_ref, where_ref = refs[:2]
        piece_refs = refs[4 : 4 + pieces_n]
        out_ref, compact, total, staged, sems = refs[4 + pieces_n :]
        first_x = (lax.axis_index("rep") * lax.axis_size("pix") + lax.axis_index("pix")) * count_x
        first_z = lax.axis_index("slab") * planes
        tiles_max = segments * GROUP // TILE
        counts_at = segments + steps * tiles_max
        copy_groups(info_ref, compact, piece_refs, first_segment, segments, batch * planes // GROUP)

        def out_copy(step, slot):
            rows = pl.ds(step * row_block, row_block)
            return pltpu.make_async_copy(staged.at[slot], out_ref.at[rows], sems.at[slot])

        shape = (row_block, planes, columns)

        def one_step(step, written):
            slot = written & 3

            def weights(tile):
                lanes = pl.ds(pl.multiple_of(tile * TILE, TILE), TILE)
                lower_x, part_x = where_ref[0:1, lanes], where_ref[1:2, lanes]
                lower_z, part_z = where_ref[2:3, lanes], where_ref[3:4, lanes]
                at_x = first_x + step * row_block + lax.broadcasted_iota(jnp.int32, (row_block, TILE), 0)
                at_z = first_z + lax.broadcasted_iota(jnp.int32, (planes, TILE), 0)
                weight_x = corner(at_x.astype(jnp.float32), lower_x, part_x)
                weight_z = corner(at_z.astype(jnp.float32), lower_z, part_z)
                matrix = (weight_x[:, None, :] * weight_z[None, :, :]).astype(jnp.bfloat16)
                return matrix.reshape(row_block * planes, TILE), lanes

            def product(tile):
                matrix, rows = weights(tile)
                return jnp.dot(matrix, compact[rows, :], preferred_element_type=jnp.float32)

            def finish(tiles):
                factors = [weights(tile) for tile in tiles]

                def part(k):
                    sums = [
                        jnp.dot(matrix, compact[rows, k * columns : (k + 1) * columns], preferred_element_type=jnp.float32)
                        for matrix, rows in factors
                    ]
                    return sum(sums[1:], sums[0])

                scale = 1.0 / (part(2) + 1.0)
                for k in range(2):
                    staged[slot, :, :, k * columns : (k + 1) * columns] = (part(k) * scale).reshape(shape)

            touched = info_ref[counts_at + step]
            list_at = segments + step * tiles_max

            @pl.when((touched > 0) & (written >= 4))
            def _():
                out_copy(step, slot).wait()

            @pl.when(touched == 1)
            def _():
                finish([info_ref[list_at]])

            @pl.when(touched == 2)
            def _():
                finish([info_ref[list_at], info_ref[list_at + 1]])

            @pl.when(touched == 3)
            def _():
                finish([info_ref[list_at + index] for index in range(3)])

            @pl.when(touched >= 4)
            def _():
                total[...] = product(info_ref[list_at]) + product(info_ref[list_at + 1])

                def add(index, carry):
                    total[...] += product(info_ref[list_at + index])
                    return carry

                lax.fori_loop(2, touched, add, 0)
                scale = 1.0 / (total[:, 2 * columns :] + 1.0)
                staged[slot, :, :, :columns] = (total[:, :columns] * scale).reshape(shape)
                staged[slot, :, :, columns:] = (total[:, columns : 2 * columns] * scale).reshape(shape)

            @pl.when(touched > 0)
            def _():
                out_copy(step, slot).start()

            return written + jnp.where(touched > 0, 1, 0)

        written = lax.fori_loop(0, steps, one_step, jnp.int32(0))
        for slot in range(4):

            @pl.when(written > slot)
            def _(slot=slot):
                out_copy(0, slot).wait()

    smem, vmem = pl.BlockSpec(memory_space=pltpu.SMEM), pl.BlockSpec(memory_space=pltpu.VMEM)
    return pl.pallas_call(
        kernel,
        out_shape=[
            jax.ShapeDtypeStruct((count_x, planes, 2 * columns), jnp.float32),
            jax.ShapeDtypeStruct(compact.shape, compact.dtype),
        ],
        in_specs=[smem, vmem, vmem, pl.BlockSpec(memory_space=pl.ANY)] + [vmem] * pieces_n,
        out_specs=[pl.BlockSpec(memory_space=pl.ANY), vmem],
        input_output_aliases={2: 1, 3: 0},
        scratch_shapes=[
            pltpu.VMEM((row_block * planes, channels), jnp.float32),
            pltpu.VMEM((4, row_block, planes, 2 * columns), jnp.float32),
            pltpu.SemaphoreType.DMA((4,)),
        ],
        compiler_params=pltpu.CompilerParams(vmem_limit_bytes=14 << 20),
        name="spread",
    )(info, where, compact, density, *pieces)[0]


def make_body(ports):
    def body(projections, ctf_weight, orient, angle_table):
        batch, planes = projections.shape[:2]
        columns = projections.shape[2] // 2
        count_x = columns // (ports.rep * ports.pix)
        row_block = TILE // planes
        sizes = (batch, planes, columns, count_x, row_block, ports.rep * ports.pix)
        samples = jnp.concatenate([projections, ctf_weight], axis=2).reshape(batch * planes, 3 * columns)
        pieces, owners, orients, orient_owners = gather_pieces(samples, orient, ports)
        info, where, density = make_plan(
            ports, orients, ports.distances(orient_owners), angle_table, ports.distances(owners), sizes
        )
        segments = owners.shape[-1] * (batch * planes // GROUP)
        compact = collect(pieces[:-1], info, segments, sizes)
        return spread(compact, density, pieces[-1:], info, where, segments, sizes)

    return body


def plain_body(projections, ctf_weight, orient, angle_table):
    planes = projections.shape[1]
    columns = projections.shape[2] // 2
    owned_rows = columns // (lax.axis_size("rep") * lax.axis_size("pix"))
    first_z = lax.axis_index("slab") * planes
    first_x = (lax.axis_index("rep") * lax.axis_size("pix") + lax.axis_index("pix")) * owned_rows
    samples = jnp.concatenate([projections, ctf_weight], axis=2)
    samples = lax.all_gather(samples, "slab", axis=1, tiled=True)
    samples = lax.all_gather(samples, BATCH_AXES, axis=0, tiled=True)
    geometry = lookup(lax.all_gather(orient, BATCH_AXES, axis=0, tiled=True), angle_table)
    geometry = geometry.astype(jnp.float32)
    at_x = (first_x + lax.iota(jnp.int32, owned_rows)).astype(jnp.float32)[:, None, None]
    at_z = (first_z + lax.iota(jnp.int32, planes)).astype(jnp.float32)[:, None, None]
    weight_x = corner(at_x, geometry[None, :, 0], geometry[None, :, 1] / 256.0)
    weight_z = corner(at_z, geometry[None, :, 2], geometry[None, :, 3] / 256.0)
    matrix = (weight_x[:, None] * weight_z[None]).astype(jnp.bfloat16).reshape(owned_rows * planes, -1)
    volume = jnp.dot(matrix, samples.reshape(-1, 3 * columns), preferred_element_type=jnp.float32)
    values = volume[:, : 2 * columns].reshape(-1, 2, columns) / (volume[:, None, 2 * columns :] + 1.0)
    return values.reshape(owned_rows, planes, 2 * columns)


def solution(mesh):
    placed = (
        P(BATCH_AXES, "slab", None),
        P(BATCH_AXES, "slab", None),
        P(BATCH_AXES),
        P(),
    )
    ports = Ports(mesh)

    def shard(body):
        return jax.shard_map(
            body, mesh=mesh, in_specs=placed, out_specs=P(BATCH_AXES, "slab", None), check_vma=False
        )

    if not ports.fits():
        return shard(plain_body)
    return shard(make_body(ports))
```
